128 devices in a mesh: gen: 16 (over x, z_hi, core), tp: 8 (over y, z_lo).
Axes of the slice: x: 4, y: 4, z: 4 (z_hi: 2, z_lo: 2; z = z_hi * 2 + z_lo), core: 2. Of those that a mesh axis runs over, the one named last changes fastest.
Arguments:
- hidden_in: bfloat16 [4, 32, 8192], P(None, 'gen'), may hold values from -6 to 6
- norm_gain: bfloat16 [8192], replicated, may hold values from 0.099609375 to 1.8984375
- w_query: bfloat16 [8192, 4096], P(('gen', 'tp')), may hold values from -0.0625 to 0.0625
- key_weight_matrix: bfloat16 [8192, 1024], P(('gen', 'tp')), may hold values from -0.0625 to 0.0625
- value_weight_matrix: bfloat16 [8192, 1024], P(('gen', 'tp')), may hold values from -0.0625 to 0.0625
- bias_query: bfloat16 [4096], P('tp'), may hold values from -3 to 3
- key_bias_vector: bfloat16 [1024], P('tp'), may hold values from -3 to 3
- value_bias_vector: bfloat16 [1024], P('tp'), may hold values from -3 to 3
- w_out: bfloat16 [4096, 8192], P(None, ('gen', 'tp')), may hold values from -0.09375 to 0.09375
- key_cache: bfloat16 [32, 8, 16384, 128], P('gen', 'tp'), may hold values from -400 to 400
- value_cache: bfloat16 [32, 8, 16384, 128], P('gen', 'tp'), may hold values from -16 to 16
- lengths: int32 [32], P('gen'), may hold values from 1 to 16384
- finished: int32 [32], P('gen'), may hold values 0 or 1
Outputs:
- layer_out: bfloat16 [4, 32, 8192], P(None, 'gen')
The draws below stay inside these ranges and needn't reach their ends.
All inputs are finite; a program needn't handle non-finite values. No bound on the sum of `finished` on one device may be relied on, other than what follows from the above.
Results may differ from the reference program's by a relative error of at most 0.012.
Values may be sent and summed in bfloat16 or wider, within the bound.
A program may use at most 128 MiB of HBM per device.

```python
import math
import jax
import jax.numpy as jnp
from jax import lax

MODEL_DIM = 8192
HQ = 32
KEY_HEADS = 8
HEAD_SIZE = 128
QUERY_GROUP = 4
CACHE_SLOTS = 16384
DECODE_STEPS = 4
ROLLOUT_ROWS = 32


def draw_key_cache(key, part):
    first_term = jax.random.fold_in(jax.random.fold_in(key, 17), 0)
    base_values = jax.random.normal(first_term, (ROLLOUT_ROWS, KEY_HEADS, CACHE_SLOTS, HEAD_SIZE), jnp.float32) * 1.8
    return jnp.clip(base_values, -400.0, 400.0).astype(jnp.bfloat16)


def draw_value_cache(key, part):
    first_term, second_term = jax.random.split(jax.random.fold_in(key, 29), 2)
    center_point = jax.random.normal(first_term, (ROLLOUT_ROWS, KEY_HEADS, 1, HEAD_SIZE), jnp.float32)
    rough_values = jax.random.normal(second_term, (ROLLOUT_ROWS, KEY_HEADS, CACHE_SLOTS, HEAD_SIZE), jnp.float32)
    values = center_point + rough_values
    return jnp.clip(values, -16.0, 16.0).astype(jnp.bfloat16)


def set_ends(drawn, stream_key, smallest, largest):
    dims = drawn.shape
    spot = [jax.random.randint(jax.random.fold_in(stream_key, axis), (), 0, dims[axis]) for axis in range(len(dims))]
    drawn = drawn.at[tuple(spot)].set(smallest)
    longest = dims.index(max(dims))
    spot[longest] = (spot[longest] + 1) % dims[longest]
    return drawn.at[tuple(spot)].set(largest)


def steps_of(key, dims, cuts, smallest, largest):
    def one(position, parts):
        steps = jax.random.uniform(jax.random.fold_in(jax.random.fold_in(key, 6), position), (parts,), jnp.float32, smallest / len(cuts), largest / len(cuts))
        return jnp.repeat(jnp.exp(steps), dims[position] // parts).reshape((-1,) + (1,) * (len(dims) - position - 1))

    factor_of = one(*cuts[0])
    for cut in cuts[1:]:
        factor_of = factor_of * one(*cut)
    return factor_of


def normal_values(own_key, dims, deviation, reach, cuts=(), kind=jnp.bfloat16):
    loudness = steps_of(own_key, dims, cuts, -0.22, 0.18) if cuts else 1.0
    array = jax.random.normal(own_key, dims, jnp.float32) * deviation * loudness
    return jnp.minimum(jnp.maximum(array, -reach), reach).astype(kind)


def setup_inputs(seed: int = 0) -> dict:
    key_list = jax.random.split(jax.random.key(seed), 14)
    hidden_in = normal_values(key_list[0], (DECODE_STEPS, ROLLOUT_ROWS, MODEL_DIM), 1.0, 6.0, ((1, 16),))
    norm_gain = jnp.clip(1.0 + 0.18 * jax.random.normal(key_list[1], (MODEL_DIM,), jnp.float32), 0.099609375, 1.8984375).astype(jnp.bfloat16)
    w_query = normal_values(key_list[2], (MODEL_DIM, HQ * HEAD_SIZE), MODEL_DIM ** -0.5, 0.0625, ((0, 128),))
    key_weight_matrix = normal_values(key_list[3], (MODEL_DIM, KEY_HEADS * HEAD_SIZE), MODEL_DIM ** -0.5, 0.0625, ((0, 128),))
    value_weight_matrix = normal_values(key_list[4], (MODEL_DIM, KEY_HEADS * HEAD_SIZE), MODEL_DIM ** -0.5, 0.0625, ((0, 128),))
    bias_query = normal_values(key_list[5], (HQ * HEAD_SIZE,), 0.5, 3.0, ((0, 8),))
    key_bias_vector = normal_values(key_list[6], (KEY_HEADS * HEAD_SIZE,), 0.5, 3.0, ((0, 8),))
    value_bias_vector = normal_values(key_list[7], (KEY_HEADS * HEAD_SIZE,), 0.5, 3.0, ((0, 8),))
    w_out = normal_values(key_list[8], (HQ * HEAD_SIZE, MODEL_DIM), (HQ * HEAD_SIZE) ** -0.5, 0.09375, ((1, 128),))
    key_cache = draw_key_cache(jax.random.fold_in(key_list[13], 71), 0)
    value_cache = draw_value_cache(jax.random.fold_in(key_list[13], 71), 0)
    lengths = set_ends(jax.random.randint(key_list[11], (ROLLOUT_ROWS,), 1, CACHE_SLOTS + 1), jax.random.fold_in(key_list[11], 1), 1, CACHE_SLOTS).astype(jnp.int32)
    finished = set_ends((jax.random.randint(key_list[12], (ROLLOUT_ROWS,), 0, 4) < 1).astype(jnp.int32), jax.random.fold_in(key_list[12], 1), 0, 1)
    return dict(hidden_in=hidden_in, norm_gain=norm_gain, w_query=w_query, key_weight_matrix=key_weight_matrix, value_weight_matrix=value_weight_matrix, bias_query=bias_query, key_bias_vector=key_bias_vector, value_bias_vector=value_bias_vector, w_out=w_out, key_cache=key_cache, value_cache=value_cache, lengths=lengths, finished=finished)


norm_eps = 1e-06
rope_base = 1000000.0
masked_score = -1e+30

def apply_rotation(values, token_positions):
    half_dim = values.shape[-1] // 2
    pair_index = jnp.arange(half_dim).astype(jnp.float32)
    frequency = jnp.exp(pair_index * (-2.0 * math.log(rope_base) / values.shape[-1]))
    angles = token_positions[..., None] * frequency
    lower_half = values[..., :half_dim]
    upper_half = values[..., half_dim:]
    cosine = jnp.cos(angles)
    sine = jnp.sin(angles)
    return jnp.concatenate([lower_half * cosine - upper_half * sine, upper_half * cosine + lower_half * sine], axis=-1)

def reference(hidden_in, norm_gain, w_query, key_weight_matrix, value_weight_matrix, bias_query, key_bias_vector, value_bias_vector, w_out, key_cache, value_cache, lengths, finished):
    widened = hidden_in.astype(jnp.float32)
    normed = widened * lax.rsqrt(lax.optimization_barrier(jnp.mean(widened * widened, axis=-1, keepdims=True)) + norm_eps) * norm_gain.astype(jnp.float32)
    flattened = normed.astype(jnp.bfloat16).reshape(DECODE_STEPS * ROLLOUT_ROWS, MODEL_DIM)
    queries = jnp.dot(flattened, w_query, preferred_element_type=jnp.float32) + bias_query.astype(jnp.float32)
    new_key_rows = jnp.dot(flattened, key_weight_matrix, preferred_element_type=jnp.float32) + key_bias_vector.astype(jnp.float32)
    fresh_value_rows = jnp.dot(flattened, value_weight_matrix, preferred_element_type=jnp.float32) + value_bias_vector.astype(jnp.float32)
    token_positions = (lengths[None, :] + jnp.arange(DECODE_STEPS, dtype=jnp.int32)[:, None]).astype(jnp.float32)[:, :, None]
    rot_query = apply_rotation(queries.reshape(DECODE_STEPS, ROLLOUT_ROWS, HQ, HEAD_SIZE), token_positions).astype(jnp.bfloat16)
    rotated_key = apply_rotation(new_key_rows.reshape(DECODE_STEPS, ROLLOUT_ROWS, KEY_HEADS, HEAD_SIZE), token_positions).astype(jnp.bfloat16)
    value_rows_new = fresh_value_rows.reshape(DECODE_STEPS, ROLLOUT_ROWS, KEY_HEADS, HEAD_SIZE).astype(jnp.bfloat16)
    score_scale = 1.0 / math.sqrt(HEAD_SIZE)
    allowed = jnp.arange(DECODE_STEPS)[None, :] <= jnp.arange(DECODE_STEPS)[:, None]

    def one_row(row_items):
        single_query_row, key_row, value_row, cache_keys, cache_values, length = row_items
        grouped_heads = single_query_row.reshape(DECODE_STEPS, KEY_HEADS, QUERY_GROUP, HEAD_SIZE).astype(jnp.float32)
        cache_scores = jnp.einsum('sjgd,jcd->sjgc', grouped_heads, cache_keys.astype(jnp.float32)) * score_scale
        inside = jnp.arange(CACHE_SLOTS) < length
        cache_scores = jnp.where(inside, cache_scores, masked_score)
        fresh_scores = jnp.einsum('sjgd,ujd->sjgu', grouped_heads, key_row.astype(jnp.float32)) * score_scale
        fresh_scores = jnp.where(allowed[:, None, None, :], fresh_scores, masked_score)
        scores = jnp.concatenate([cache_scores, fresh_scores], axis=-1)
        row_max = lax.optimization_barrier(jnp.max(scores, axis=-1, keepdims=True))
        weights = jnp.exp(scores - row_max)
        row_sum = lax.optimization_barrier(jnp.sum(weights, axis=-1))
        rounded = lax.optimization_barrier(weights.astype(jnp.bfloat16)).astype(jnp.float32)
        numerator = jnp.einsum('sjgc,jcd->sjgd', rounded[..., :CACHE_SLOTS], cache_values.astype(jnp.float32))
        numerator = numerator + jnp.einsum('sjgu,ujd->sjgd', rounded[..., CACHE_SLOTS:], value_row.astype(jnp.float32))
        return (numerator / row_sum[..., None]).astype(jnp.bfloat16).reshape(DECODE_STEPS, HQ * HEAD_SIZE)
    attended = lax.map(one_row, (jnp.transpose(rot_query, (1, 0, 2, 3)), jnp.transpose(rotated_key, (1, 0, 2, 3)), jnp.transpose(value_rows_new, (1, 0, 2, 3)), key_cache, value_cache, lengths))
    attended = jnp.transpose(attended, (1, 0, 2)).reshape(DECODE_STEPS * ROLLOUT_ROWS, HQ * HEAD_SIZE)
    projected = jnp.dot(attended, w_out, preferred_element_type=jnp.float32).reshape(DECODE_STEPS, ROLLOUT_ROWS, MODEL_DIM)
    layer_out = jnp.where(finished[None, :, None] != 0, widened, widened + projected)
    return layer_out.astype(jnp.bfloat16)
```

```python
import functools
import math

import jax
import jax.numpy as jnp
from jax import lax
from jax.experimental import pallas as pl
from jax.experimental.pallas import tpu as pltpu
from jax.sharding import PartitionSpec as P

NORM_EPS = 1e-06
ROPE_BASE = 1000000.0
MASKED = -1e30
MESH = pl.DeviceIdType.MESH
GEN, TP = 16, 8
TOK = 8
D = 8192
FB = D // GEN
HD = 128
QW = 512
CW = QW + 2 * HD
SLOTS = 16384
CHUNK = 2048
NCH = SLOTS // CHUNK
PIECES = 4
PIECE = SLOTS // PIECES


def peer(g, t):
    return {"gen": g, "tp": t}


def remote(src, dst, send_sem, recv_sem, g, t):
    return pltpu.make_async_remote_copy(
        src_ref=src, dst_ref=dst, send_sem=send_sem, recv_sem=recv_sem,
        device_id=peer(g, t), device_id_type=MESH,
    )


def kernel(
    hid, gain, wq, wk, wv, bias, wo, kc, vc, lens,
    out_ref,
    h_v, gain_v, bias_v, lens_s, hf_v,
    w_stage, w_full, o_stage, o_full, k_v, v_v,
    x_send, x_recv, p_send, p_recv, a_recv, s_v,
    r_send, r_recv, f_send, f_recv, rope_v,
    small_sem, w_sem, wo_sem, kv_sem,
    x_ss, x_rs, ws_ss, w_rs, o_ss, o_rs, p_ss, p_rs, a_ss, a_rs, r_ss, r_rs, f_ss, f_rs,
):
    g = lax.axis_index("gen")
    t = lax.axis_index("tp")
    zl = lax.rem(t, 2)
    ty = lax.div(t, 2)

    def gn(i):
        return lax.rem(g + i, GEN)

    def tn(j):
        return lax.rem(t + j, TP)

    barrier = pltpu.get_barrier_semaphore()
    for i in range(1, GEN):
        pl.semaphore_signal(barrier, inc=1, device_id=peer(gn(i), t), device_id_type=MESH)
    for j in range(1, TP):
        pl.semaphore_signal(barrier, inc=1, device_id=peer(g, tn(j)), device_id_type=MESH)

    smalls = [
        pltpu.make_async_copy(hid, h_v, small_sem.at[0]),
        pltpu.make_async_copy(gain, gain_v, small_sem.at[1]),
        pltpu.make_async_copy(bias, bias_v, small_sem.at[2]),
        pltpu.make_async_copy(lens, lens_s, small_sem.at[3]),
    ]
    for c in smalls:
        c.start()

    def w_copies(j):
        tj = tn(j)
        dst = w_full.at[t] if j == 0 else w_stage.at[j]
        return [
            pltpu.make_async_copy(wq.at[:, pl.ds(tj * QW, QW)], dst.at[:, pl.ds(0, QW)], w_sem.at[j, 0]),
            pltpu.make_async_copy(wk.at[:, pl.ds(tj * HD, HD)], dst.at[:, pl.ds(QW, HD)], w_sem.at[j, 1]),
            pltpu.make_async_copy(wv.at[:, pl.ds(tj * HD, HD)], dst.at[:, pl.ds(QW + HD, HD)], w_sem.at[j, 2]),
        ]

    def wo_copy(j):
        dst = o_full.at[t] if j == 0 else o_stage.at[j]
        return pltpu.make_async_copy(wo.at[:, pl.ds(tn(j) * QW, QW)], dst, wo_sem.at[j])

    for j in range(TP):
        for c in w_copies(j):
            c.start()
    for j in range(TP):
        wo_copy(j).start()

    def kv_copies():
        res = []
        for n, (src, dst) in enumerate(((kc, k_v), (vc, v_v))):
            for i in range(PIECES):
                for r in range(2):
                    res.append(pltpu.make_async_copy(
                        src.at[r, 0, pl.ds(i * PIECE, PIECE), :],
                        dst.at[r, pl.ds(i * PIECE, PIECE), :],
                        kv_sem.at[n, r, i],
                    ))
        return res

    for c in kv_copies():
        c.start()

    smalls[0].wait()
    smalls[1].wait()
    h = jnp.concatenate([h_v[s].astype(jnp.float32) for s in range(4)], axis=0)
    hf_v[...] = h
    scale = lax.rsqrt(jnp.mean(h * h, axis=-1, keepdims=True) + NORM_EPS)
    normed = (h * scale * gain_v[...]).astype(jnp.bfloat16)
    for i in range(GEN):
        x_send[i] = normed[:, i * FB:(i + 1) * FB]
    x_recv[g] = x_send[g]

    pl.semaphore_wait(barrier, GEN - 1 + TP - 1)

    def x_copy(i):
        return remote(x_send.at[gn(i)], x_recv.at[g], x_ss.at[i], x_rs.at[g], gn(i), t)

    def w_send(j):
        return remote(w_stage.at[j], w_full.at[t], ws_ss.at[j], w_rs.at[t], g, tn(j))

    def o_send(j):
        return remote(o_stage.at[j], o_full.at[t], o_ss.at[j], o_rs.at[t], g, tn(j))

    for i in range(1, GEN):
        x_copy(i).start()
    for j in range(1, TP):
        for c in w_copies(j):
            c.wait()
        w_send(j).start()
    for j in range(1, TP):
        wo_copy(j).wait()
        o_send(j).start()
    for c in w_copies(0):
        c.wait()
    wo_copy(0).wait()

    smalls[3].wait()
    smalls[2].wait()
    row = lax.broadcasted_iota(jnp.int32, (TOK, HD), 0)
    lane = lax.broadcasted_iota(jnp.int32, (TOK, HD), 1)
    odd = lax.rem(row, 2) == 1
    len8 = jnp.where(odd, lens_s[1], lens_s[0])
    position = (len8 + lax.div(row, 2)).astype(jnp.float32)
    pair = lax.rem(lane, HD // 2).astype(jnp.float32)
    angles = position * jnp.exp(pair * (-2.0 * math.log(ROPE_BASE) / HD))
    rope_v[0] = jnp.cos(angles)
    rope_v[1] = jnp.where(lane < HD // 2, -1.0, 1.0) * jnp.sin(angles)

    for i in range(1, GEN):
        src = gn(i)
        remote(x_send.at[src], x_recv.at[src], x_ss.at[i], x_rs.at[src], src, t).wait_recv()
    for j in range(1, TP):
        src = tn(j)
        remote(w_stage.at[j], w_full.at[src], ws_ss.at[j], w_rs.at[src], g, src).wait_recv()

    x_all = x_recv[...].reshape(GEN * TOK, FB)
    w_all = w_full[...].reshape(FB, CW)
    part = jnp.dot(x_all, w_all, preferred_element_type=jnp.float32)
    p_send[...] = part.astype(jnp.bfloat16).reshape(GEN, TOK, CW)

    def p_copy(i):
        return remote(p_send.at[gn(i)], p_recv.at[g], p_ss.at[i], p_rs.at[g], gn(i), t)

    for i in range(1, GEN):
        p_copy(i).start()
    p_recv[g] = p_send[g]
    for i in range(1, GEN):
        src = gn(i)
        remote(p_send.at[src], p_recv.at[src], p_ss.at[i], p_rs.at[src], src, t).wait_recv()
    for c in kv_copies():
        c.wait()

    qkv = jnp.sum(p_recv[...].astype(jnp.float32), axis=0) + bias_v[...]
    cosine = rope_v[0]
    sine = rope_v[1]

    def rotated(x):
        return x * cosine + pltpu.roll(x, HD // 2, axis=1) * sine

    q = jnp.concatenate([rotated(qkv[:, n * HD:(n + 1) * HD]) for n in range(4)], axis=0)
    k_new = rotated(qkv[:, QW:QW + HD]).astype(jnp.bfloat16)
    v_new = qkv[:, QW + HD:].astype(jnp.bfloat16)
    qrow = lax.broadcasted_iota(jnp.int32, (4 * TOK, HD), 0)
    q_odd = lax.rem(qrow, 2) == 1
    q_both = jnp.concatenate(
        [jnp.where(q_odd, 0.0, q), jnp.where(q_odd, q, 0.0)], axis=1
    ).astype(jnp.bfloat16)
    q16 = q.astype(jnp.bfloat16)
    nt = (((1,), (1,)), ((), ()))
    qlen = jnp.where(lax.rem(lax.broadcasted_iota(jnp.int32, (4 * TOK, CHUNK), 0), 2) == 1, lens_s[1], lens_s[0])
    places = lax.broadcasted_iota(jnp.int32, (4 * TOK, CHUNK), 1)

    fresh = lax.dot_general(q16, k_new, nt, preferred_element_type=jnp.float32)
    fq = lax.rem(lax.broadcasted_iota(jnp.int32, (4 * TOK, TOK), 0), TOK)
    fk = lax.broadcasted_iota(jnp.int32, (4 * TOK, TOK), 1)
    seen = (lax.rem(fq, 2) == lax.rem(fk, 2)) & (lax.div(fk, 2) <= lax.div(fq, 2))
    fresh = jnp.where(seen, fresh, MASKED)

    def score(c, top):
        at = pl.multiple_of(c * CHUNK, CHUNK)
        keys = jnp.concatenate([k_v[0, pl.ds(at, CHUNK), :], k_v[1, pl.ds(at, CHUNK), :]], axis=1)
        s = lax.dot_general(q_both, keys, nt, preferred_element_type=jnp.float32)
        s = jnp.where(places < qlen - at, s, MASKED)
        s_v[c] = s
        for n in range(CHUNK // HD):
            top = jnp.maximum(top, s[:, n * HD:(n + 1) * HD])
        return top

    top = lax.fori_loop(0, NCH, score, jnp.full((4 * TOK, HD), MASKED, jnp.float32))
    top = jnp.maximum(jnp.max(top, axis=1, keepdims=True), jnp.max(fresh, axis=1, keepdims=True))
    to_exp = 1.0 / math.sqrt(HD)

    def weigh(c, carry):
        total, acc = carry
        at = pl.multiple_of(c * CHUNK, CHUNK)
        w = jnp.exp((s_v[c] - top) * to_exp)
        for n in range(CHUNK // HD):
            total = total + w[:, n * HD:(n + 1) * HD]
        values = jnp.concatenate([v_v[0, pl.ds(at, CHUNK), :], v_v[1, pl.ds(at, CHUNK), :]], axis=1)
        acc = acc + jnp.dot(w.astype(jnp.bfloat16), values, preferred_element_type=jnp.float32)
        return total, acc

    total, acc = lax.fori_loop(
        0, NCH, weigh,
        (jnp.zeros((4 * TOK, HD), jnp.float32), jnp.zeros((4 * TOK, 2 * HD), jnp.float32)),
    )
    fw = jnp.exp((fresh - top) * to_exp)
    denom = jnp.sum(total, axis=1, keepdims=True) + jnp.sum(fw, axis=1, keepdims=True)
    num = jnp.where(q_odd, acc[:, HD:], acc[:, :HD])
    num = num + jnp.dot(fw.astype(jnp.bfloat16), v_new, preferred_element_type=jnp.float32)
    att = num / denom
    a_recv[g] = jnp.concatenate([att[n * TOK:(n + 1) * TOK] for n in range(4)], axis=1).astype(jnp.bfloat16)

    def a_copy(i):
        return remote(a_recv.at[g], a_recv.at[g], a_ss.at[i], a_rs.at[g], gn(i), t)

    for i in range(1, GEN):
        a_copy(i).start()
    for j in range(1, TP):
        src = tn(j)
        remote(o_stage.at[j], o_full.at[src], o_ss.at[j], o_rs.at[src], g, src).wait_recv()
    for i in range(1, GEN):
        src = gn(i)
        remote(a_recv.at[g], a_recv.at[src], a_ss.at[i], a_rs.at[src], src, t).wait_recv()

    a_all = a_recv[...].reshape(GEN * TOK, QW)
    o_all = o_full[...].reshape(QW, QW)
    outp = lax.dot_general(a_all, o_all, nt, preferred_element_type=jnp.float32)
    for z in range(2):
        for y in range(4):
            r_send[2 * y + z] = outp[64 * z:64 * z + 64, HD * y:HD * y + HD].astype(jnp.bfloat16)

    def r_copy(j):
        return remote(r_send.at[tn(j)], r_recv.at[t], r_ss.at[j], r_rs.at[t], g, tn(j))

    for j in range(1, TP):
        r_copy(j).start()
    r_recv[t] = r_send[t]
    for j in range(1, TP):
        src = tn(j)
        remote(r_send.at[src], r_recv.at[src], r_ss.at[j], r_rs.at[src], g, src).wait_recv()
    full = jnp.sum(r_recv[...].astype(jnp.float32), axis=0).astype(jnp.bfloat16)
    f_send[...] = full.reshape(8, TOK, HD)

    def f_copy(n, j):
        return remote(
            f_send.at[n], f_recv.at[g, ty], f_ss.at[n, j], f_rs.at[g, ty], zl * 8 + n, tn(j)
        )

    own_half = lax.div(g, 8)

    def each_send(act):
        for n in range(8):
            for j in range(TP):
                if j == 0:
                    @pl.when(zl * 8 + n != g)
                    def _():
                        act(f_copy(n, j))
                else:
                    act(f_copy(n, j))

    each_send(lambda c: c.start())

    @pl.when(zl == own_half)
    def _():
        f_recv[g, ty] = f_send[lax.rem(g, 8)]

    for gs in range(GEN):
        for ys in range(4):
            def wait_one(gs=gs, ys=ys):
                remote(
                    f_send.at[0], f_recv.at[gs, ys], f_ss.at[0, 0], f_rs.at[gs, ys],
                    gs, ys * 2 + own_half,
                ).wait_recv()

            @pl.when(jnp.logical_not((g == gs) & (t == ys * 2 + own_half)))
            def _():
                wait_one()

    for c in range(GEN * 4):
        cols = slice(c * HD, (c + 1) * HD)
        block = f_recv[c // 4, c % 4].astype(jnp.float32)
        keep = jnp.where(odd, lens_s[3], lens_s[2]) != 0
        mine = hf_v[:, cols]
        hf_v[:, cols] = jnp.where(keep, mine, mine + block)
    for s in range(4):
        out_ref[s] = hf_v[2 * s:2 * s + 2, :].astype(jnp.bfloat16)

    for i in range(1, GEN):
        x_copy(i).wait_send()
        p_copy(i).wait_send()
        a_copy(i).wait_send()
    for j in range(1, TP):
        w_send(j).wait_send()
        o_send(j).wait_send()
        r_copy(j).wait_send()
    each_send(lambda c: c.wait_send())


def shards(
    hidden_in, norm_gain, w_query, key_weight_matrix, value_weight_matrix, bias_query,
    key_bias_vector, value_bias_vector, w_out, key_cache, value_cache, lengths, finished,
):
    gain = norm_gain.astype(jnp.float32).reshape(1, D)
    bias = jnp.concatenate([bias_query, key_bias_vector, value_bias_vector]).astype(jnp.float32).reshape(1, CW)
    info = jnp.concatenate([lengths, finished])
    any_ = pl.BlockSpec(memory_space=pl.ANY)
    bf16, f32 = jnp.bfloat16, jnp.float32
    dma = pltpu.SemaphoreType.DMA
    return pl.pallas_call(
        kernel,
        out_shape=jax.ShapeDtypeStruct((4, 2, D), bf16),
        in_specs=[any_] * 10,
        out_specs=pl.BlockSpec(memory_space=pltpu.VMEM),
        scratch_shapes=[
            pltpu.VMEM((4, 2, D), bf16),
            pltpu.VMEM((1, D), f32),
            pltpu.VMEM((1, CW), f32),
            pltpu.SMEM((4,), jnp.int32),
            pltpu.VMEM((TOK, D), f32),
            pltpu.VMEM((TP, 64, CW), bf16),
            pltpu.VMEM((TP, 64, CW), bf16),
            pltpu.VMEM((TP, 64, QW), bf16),
            pltpu.VMEM((TP, 64, QW), bf16),
            pltpu.VMEM((2, SLOTS, HD), bf16),
            pltpu.VMEM((2, SLOTS, HD), bf16),
            pltpu.VMEM((GEN, TOK, FB), bf16),
            pltpu.VMEM((GEN, TOK, FB), bf16),
            pltpu.VMEM((GEN, TOK, CW), bf16),
            pltpu.VMEM((GEN, TOK, CW), bf16),
            pltpu.VMEM((GEN, TOK, QW), bf16),
            pltpu.VMEM((NCH, 4 * TOK, CHUNK), f32),
            pltpu.VMEM((TP, 64, HD), bf16),
            pltpu.VMEM((TP, 64, HD), bf16),
            pltpu.VMEM((8, TOK, HD), bf16),
            pltpu.VMEM((GEN, 4, TOK, HD), bf16),
            pltpu.VMEM((2, TOK, HD), f32),
            dma((4,)),
            dma((TP, 3)),
            dma((TP,)),
            dma((2, 2, PIECES)),
            dma((GEN,)), dma((GEN,)),
            dma((TP,)), dma((TP,)),
            dma((TP,)), dma((TP,)),
            dma((GEN,)), dma((GEN,)),
            dma((GEN,)), dma((GEN,)),
            dma((TP,)), dma((TP,)),
            dma((8, TP)), dma((GEN, 4)),
        ],
        compiler_params=pltpu.CompilerParams(
            collective_id=0, has_side_effects=True, vmem_limit_bytes=60 * 1024 * 1024
        ),
        name="layer",
    )(
        hidden_in, gain, w_query, key_weight_matrix, value_weight_matrix, bias, w_out.T,
        key_cache, value_cache, info,
    )


def solution(mesh):
    placed = (
        P(None, "gen", None),
        P(),
        P(("gen", "tp"), None),
        P(("gen", "tp"), None),
        P(("gen", "tp"), None),
        P("tp"),
        P("tp"),
        P("tp"),
        P(None, ("gen", "tp")),
        P("gen", "tp", None, None),
        P("gen", "tp", None, None),
        P("gen"),
        P("gen"),
    )
    return jax.shard_map(
        shards, mesh=mesh, in_specs=placed, out_specs=P(None, "gen", None), check_vma=False
    )
```

```python
import functools
import math

import jax
import jax.numpy as jnp
from jax import lax
from jax.experimental import pallas as pl
from jax.experimental.pallas import tpu as pltpu
from jax.sharding import PartitionSpec as P

NORM_EPS = 1e-06
ROPE_BASE = 1000000.0
MASKED = -1e30
MESH = pl.DeviceIdType.MESH
GEN, TP = 16, 8
TOK = 8
D = 8192
FB = D // GEN
HD = 128
QW = 512
CW = QW + 2 * HD
SLOTS = 16384
CHUNK = 2048
NCH = SLOTS // CHUNK
PIECES = 4
PIECE = SLOTS // PIECES


def peer(g, t):
    return {"gen": g, "tp": t}


def remote(src, dst, send_sem, recv_sem, g, t):
    return pltpu.make_async_remote_copy(
        src_ref=src, dst_ref=dst, send_sem=send_sem, recv_sem=recv_sem,
        device_id=peer(g, t), device_id_type=MESH,
    )


class Phase:
    def __init__(self):
        self.now = None

    def __call__(self, name):
        if self.now is not None:
            self.now.__exit__(None, None, None)
        self.now = jax.named_scope(name) if name else None
        if name:
            self.now.__enter__()


def kernel(
    hid, gain, wq, wk, wv, bq, bk, bv, wo, kc, vc, lens, fin,
    out_ref,
    h_v, gain_v, bq_v, bk_v, bv_v, lens_s, fin_s, hf_v, m_v,
    wa_stage, wb_stage, wa_full, wb_full, o_stage, o_full, k_v, v_v, kt_v,
    x_send, x_recv, pa_send, pb_send, pa_recv, pb_recv, a_recv, s_v,
    r_send, r_recv, f_send, f_recv, rope_v,
    small_sem, w_sem, wo_sem, kv_sem,
    x_ss, x_rs, wa_ss, wa_rs, wb_ss, wb_rs, o_ss, o_rs, pa_ss, pa_rs, pb_ss, pb_rs,
    a_ss, a_rs, r_ss, r_rs, f_ss, f_rs,
):
    ph = Phase()
    g = lax.axis_index("gen")
    t = lax.axis_index("tp")
    x, zh, core = lax.div(g, 4), lax.rem(lax.div(g, 2), 2), lax.rem(g, 2)
    ty, zl = lax.div(t, 2), lax.rem(t, 2)
    pa = 2 * ty + core
    pb = 2 * x + core

    def gn(i):
        return lax.rem(g + i, GEN)

    def tn(j):
        return lax.rem(t + j, TP)

    def an(j):
        p = lax.rem(pa + j, TP)
        return p, g - core + lax.rem(p, 2), 2 * lax.div(p, 2) + zl

    def bn(j):
        p = lax.rem(pb + j, TP)
        return p, 4 * lax.div(p, 2) + 2 * zh + lax.rem(p, 2), t

    ph("issue")
    barrier = pltpu.get_barrier_semaphore()

    def greet(gg, tt):
        pl.semaphore_signal(barrier, inc=1, device_id=peer(gg, tt), device_id_type=MESH)

    for i in range(1, GEN):
        greet(gn(i), t)
    for j in range(1, TP):
        greet(g, tn(j))
    for k in range(1, 4):
        greet(g - core + (1 - core), lax.rem(t + 2 * k, TP))

    smalls = [
        pltpu.make_async_copy(src, dst, small_sem.at[n])
        for n, (src, dst) in enumerate((
            (hid, h_v), (gain, gain_v), (bq, bq_v), (bk, bk_v), (bv, bv_v), (lens, lens_s), (fin, fin_s),
        ))
    ]
    for c in smalls:
        c.start()

    def wa_copy(j):
        p = lax.rem(pa + j, TP)
        dst = wa_full if j == 0 else wa_stage
        return pltpu.make_async_copy(wq.at[:, pl.ds(p * QW, QW)], dst.at[p], w_sem.at[p, 0])

    def wb_copies(j):
        p = lax.rem(pb + j, TP)
        dst = (wb_full if j == 0 else wb_stage).at[p]
        return [
            pltpu.make_async_copy(src.at[:, pl.ds(p * HD, HD)], dst.at[:, pl.ds(n * HD, HD)], w_sem.at[p, 1 + n])
            for n, src in enumerate((wk, wv))
        ]

    def wo_copy(j):
        dst = o_full.at[t] if j == 0 else o_stage.at[j]
        return pltpu.make_async_copy(wo.at[:, pl.ds(tn(j) * QW, QW)], dst, wo_sem.at[j])

    for j in range(TP):
        wa_copy(j).start()
        for c in wb_copies(j):
            c.start()

    def kv_copy(n, r, i):
        src, dst = ((kc, k_v), (vc, v_v))[n]
        return pltpu.make_async_copy(
            src.at[r, 0, pl.ds(i * PIECE, PIECE), :],
            dst.at[r, pl.ds(i * PIECE, PIECE), :],
            kv_sem.at[n, r, i],
        )

    ph("norm")
    smalls[0].wait()
    smalls[1].wait()
    h = jnp.concatenate([h_v[s].astype(jnp.float32) for s in range(4)], axis=0)
    hf_v[...] = h
    scale = lax.rsqrt(jnp.mean(h * h, axis=-1, keepdims=True) + NORM_EPS)
    normed = h * scale * gain_v[...].astype(jnp.float32).reshape(1, D)
    row = lax.broadcasted_iota(jnp.int32, (TOK, HD), 0)
    lane = lax.broadcasted_iota(jnp.int32, (TOK, HD), 1)
    stays = (lane < 64) == (zl == 0)
    for n in range(8):
        for m in range(4):
            c0 = normed[:, (8 * n + m) * HD:(8 * n + m + 1) * HD]
            c1 = normed[:, (8 * n + 4 + m) * HD:(8 * n + 5 + m) * HD]
            moved = pltpu.roll(jnp.where(zl == 0, c1, c0), 64, axis=1)
            both = jnp.where(stays, jnp.where(zl == 0, c0, c1), moved)
            m_v[n, m] = both
            x_send[n, :, m * HD:(m + 1) * HD] = both.astype(jnp.bfloat16)
    for z in range(2):
        for m in range(4):
            block = m_v[2 * m + z, ty].astype(jnp.bfloat16)
            for n in range(4):
                x_send[2 * n + z, :, FB + m * HD:FB + (m + 1) * HD] = block
    x_recv[g] = x_send[lax.div(g, 2)]

    ph("barrier")
    pl.semaphore_wait(barrier, GEN - 1 + TP - 1 + 3)
    ph("send_xw")

    def x_copy(i):
        return remote(x_send.at[lax.div(gn(i), 2)], x_recv.at[g], x_ss.at[i], x_rs.at[g], gn(i), t)

    def wa_send(j):
        p, gg, tt = an(j)
        return remote(wa_stage.at[p], wa_full.at[pa], wa_ss.at[j], wa_rs.at[pa], gg, tt)

    def wb_send(j):
        p, gg, tt = bn(j)
        return remote(wb_stage.at[p], wb_full.at[pb], wb_ss.at[j], wb_rs.at[pb], gg, tt)

    def o_send(j):
        return remote(o_stage.at[j], o_full.at[t], o_ss.at[j], o_rs.at[t], g, tn(j))

    for i in range(1, GEN):
        x_copy(i).start()
    for j in range(1, TP):
        wa_copy(j).wait()
        wa_send(j).start()
        for c in wb_copies(j):
            c.wait()
        wb_send(j).start()
    wa_copy(0).wait()
    for c in wb_copies(0):
        c.wait()
    for n in range(2):
        for i in range(PIECES):
            for r in range(2):
                kv_copy(n, r, i).start()
    for j in range(TP):
        wo_copy(j).start()

    ph("rope")
    for c in smalls[2:]:
        c.wait()
    odd = lax.rem(row, 2) == 1
    len8 = jnp.where(odd, lens_s[1], lens_s[0])
    position = (len8 + lax.div(row, 2)).astype(jnp.float32)
    pair = lax.rem(lane, HD // 2).astype(jnp.float32)
    angles = position * jnp.exp(pair * (-2.0 * math.log(ROPE_BASE) / HD))
    rope_v[0] = jnp.cos(angles)
    rope_v[1] = jnp.where(lane < HD // 2, -1.0, 1.0) * jnp.sin(angles)

    ph("turn_k")
    nt = (((1,), (1,)), ((), ()))
    er = lax.broadcasted_iota(jnp.int32, (2 * HD, 2 * HD), 0)
    ec = lax.broadcasted_iota(jnp.int32, (2 * HD, 2 * HD), 1)
    eye = jnp.where(er == ec, 1.0, 0.0).astype(jnp.bfloat16)
    per = PIECE // CHUNK
    for i in range(PIECES):
        for r in range(2):
            kv_copy(0, r, i).wait()

        def turn(c, carry):
            at = pl.multiple_of(c * CHUNK, CHUNK)
            keys = jnp.concatenate([k_v[0, pl.ds(at, CHUNK), :], k_v[1, pl.ds(at, CHUNK), :]], axis=1)
            kt_v[c] = lax.dot_general(eye, keys, nt, preferred_element_type=jnp.float32).astype(jnp.bfloat16)
            return carry

        lax.fori_loop(i * per, (i + 1) * per, turn, 0)

    ph("wait_x")
    for i in range(1, GEN):
        src = gn(i)
        remote(x_send.at[0], x_recv.at[src], x_ss.at[i], x_rs.at[src], src, t).wait_recv()
    ph("wait_wa")
    for j in range(1, TP):
        p, gg, tt = an(j)
        remote(wa_stage.at[p], wa_full.at[p], wa_ss.at[j], wa_rs.at[p], gg, tt).wait_recv()
    ph("qkv")
    part = jnp.dot(
        x_recv[:, :, :FB].reshape(GEN * TOK, FB), wa_full[...].reshape(FB, QW),
        preferred_element_type=jnp.float32,
    )
    pa_send[...] = part.astype(jnp.bfloat16).reshape(GEN, TOK, QW)

    slot_a = 4 * x + 2 * zh + zl
    slot_b = 4 * ty + 2 * zh + zl

    def pa_copy(i):
        return remote(pa_send.at[gn(i)], pa_recv.at[slot_a], pa_ss.at[i], pa_rs.at[slot_a], gn(i), pa)

    def pb_copy(i):
        return remote(pb_send.at[gn(i)], pb_recv.at[slot_b], pb_ss.at[i], pb_rs.at[slot_b], gn(i), pb)

    def unless(own, act):
        @pl.when(jnp.logical_not(own))
        def _():
            act()

    own_a = zl == core
    own_b = t == pb
    for i in range(1, GEN):
        pa_copy(i).start()
    unless(own_a, lambda: pa_copy(0).start())

    @pl.when(own_a)
    def _():
        pa_recv[slot_a] = pa_send[g]

    ph("wait_wb")
    for j in range(1, TP):
        p, gg, tt = bn(j)
        remote(wb_stage.at[p], wb_full.at[p], wb_ss.at[j], wb_rs.at[p], gg, tt).wait_recv()
    ph("kvp")
    part = jnp.dot(
        x_recv[:, :, FB:].reshape(GEN * TOK, FB), wb_full[...].reshape(FB, 2 * HD),
        preferred_element_type=jnp.float32,
    )
    pb_send[...] = part.astype(jnp.bfloat16).reshape(GEN, TOK, 2 * HD)
    for i in range(1, GEN):
        pb_copy(i).start()
    unless(own_b, lambda: pb_copy(0).start())

    @pl.when(own_b)
    def _():
        pb_recv[slot_b] = pb_send[g]

    ph("wait_p")

    def pa_wait(i):
        k = lax.rem(slot_a + i, GEN)
        gg = 4 * lax.div(k, 4) + 2 * lax.rem(lax.div(k, 2), 2) + zl
        remote(pa_send.at[0], pa_recv.at[k], pa_ss.at[i], pa_rs.at[k], gg, 2 * ty + lax.rem(k, 2)).wait_recv()

    def pb_wait(i):
        k = lax.rem(slot_b + i, GEN)
        gg = 4 * ty + 2 * lax.rem(lax.div(k, 2), 2) + zl
        remote(
            pb_send.at[0], pb_recv.at[k], pb_ss.at[i], pb_rs.at[k],
            gg, 2 * lax.div(k, 4) + lax.rem(k, 2),
        ).wait_recv()

    for i in range(1, GEN):
        pa_wait(i)
        pb_wait(i)
    unless(own_a, lambda: pa_wait(0))
    unless(own_b, lambda: pb_wait(0))

    ph("wait_kv")
    for j in range(1, TP):
        wo_copy(j).wait()
        o_send(j).start()
    wo_copy(0).wait()
    for i in range(PIECES):
        for r in range(2):
            kv_copy(1, r, i).wait()

    ph("head")
    cosine = rope_v[0]
    sine = rope_v[1]

    def rotated(v):
        return v * cosine + pltpu.roll(v, HD // 2, axis=1) * sine

    qs = jnp.sum(pa_recv[...].astype(jnp.float32), axis=0) + bq_v[...].astype(jnp.float32).reshape(1, QW)
    kvs = jnp.sum(pb_recv[...].astype(jnp.float32), axis=0)
    q = jnp.concatenate([rotated(qs[:, n * HD:(n + 1) * HD]) for n in range(4)], axis=0)
    k_new = rotated(kvs[:, :HD] + bk_v[...].astype(jnp.float32).reshape(1, HD)).astype(jnp.bfloat16)
    v_new = (kvs[:, HD:] + bv_v[...].astype(jnp.float32).reshape(1, HD)).astype(jnp.bfloat16)
    qrow = lax.broadcasted_iota(jnp.int32, (4 * TOK, HD), 0)
    q_odd = lax.rem(qrow, 2) == 1
    q_both = jnp.concatenate(
        [jnp.where(q_odd, 0.0, q), jnp.where(q_odd, q, 0.0)], axis=1
    ).astype(jnp.bfloat16)
    q16 = q.astype(jnp.bfloat16)
    qlen = jnp.where(lax.rem(lax.broadcasted_iota(jnp.int32, (4 * TOK, CHUNK), 0), 2) == 1, lens_s[1], lens_s[0])
    places = lax.broadcasted_iota(jnp.int32, (4 * TOK, CHUNK), 1)

    fresh = lax.dot_general(q16, k_new, nt, preferred_element_type=jnp.float32)
    fq = lax.rem(lax.broadcasted_iota(jnp.int32, (4 * TOK, TOK), 0), TOK)
    fk = lax.broadcasted_iota(jnp.int32, (4 * TOK, TOK), 1)
    seen = (lax.rem(fq, 2) == lax.rem(fk, 2)) & (lax.div(fk, 2) <= lax.div(fq, 2))
    fresh = jnp.where(seen, fresh, MASKED)

    def score(c, top):
        at = pl.multiple_of(c * CHUNK, CHUNK)
        s = jnp.dot(q_both, kt_v[c], preferred_element_type=jnp.float32)
        s = jnp.where(places < qlen - at, s, MASKED)
        s_v[c] = s
        for n in range(CHUNK // HD):
            top = jnp.maximum(top, s[:, n * HD:(n + 1) * HD])
        return top

    ph("score")
    top = lax.fori_loop(0, NCH, score, jnp.full((4 * TOK, HD), MASKED, jnp.float32))
    top = jnp.maximum(jnp.max(top, axis=1, keepdims=True), jnp.max(fresh, axis=1, keepdims=True))
    to_exp = 1.0 / math.sqrt(HD)

    def weigh(c, carry):
        total, acc = carry
        at = pl.multiple_of(c * CHUNK, CHUNK)
        w = jnp.exp((s_v[c] - top) * to_exp)
        for n in range(CHUNK // HD):
            total = total + w[:, n * HD:(n + 1) * HD]
        values = jnp.concatenate([v_v[0, pl.ds(at, CHUNK), :], v_v[1, pl.ds(at, CHUNK), :]], axis=1)
        acc = acc + jnp.dot(w.astype(jnp.bfloat16), values, preferred_element_type=jnp.float32)
        return total, acc

    ph("weigh")
    total, acc = lax.fori_loop(
        0, NCH, weigh,
        (jnp.zeros((4 * TOK, HD), jnp.float32), jnp.zeros((4 * TOK, 2 * HD), jnp.float32)),
    )
    ph("att_end")
    fw = jnp.exp((fresh - top) * to_exp)
    denom = jnp.sum(total, axis=1, keepdims=True) + jnp.sum(fw, axis=1, keepdims=True)
    num = jnp.where(q_odd, acc[:, HD:], acc[:, :HD])
    num = num + jnp.dot(fw.astype(jnp.bfloat16), v_new, preferred_element_type=jnp.float32)
    att = num / denom
    a_recv[g] = jnp.concatenate([att[n * TOK:(n + 1) * TOK] for n in range(4)], axis=1).astype(jnp.bfloat16)

    def a_copy(i):
        return remote(a_recv.at[g], a_recv.at[g], a_ss.at[i], a_rs.at[g], gn(i), t)

    for i in range(1, GEN):
        a_copy(i).start()
    ph("wait_o")
    for j in range(1, TP):
        src = tn(j)
        remote(o_stage.at[j], o_full.at[src], o_ss.at[j], o_rs.at[src], g, src).wait_recv()
    ph("wait_a")
    for i in range(1, GEN):
        src = gn(i)
        remote(a_recv.at[g], a_recv.at[src], a_ss.at[i], a_rs.at[src], src, t).wait_recv()

    ph("outmm")
    a_all = a_recv[...].reshape(GEN * TOK, QW)
    o_all = o_full[...].reshape(QW, QW)
    outp = lax.dot_general(a_all, o_all, nt, preferred_element_type=jnp.float32)
    for z in range(2):
        for y in range(4):
            r_send[2 * y + z] = outp[64 * z:64 * z + 64, HD * y:HD * y + HD].astype(jnp.bfloat16)

    def r_copy(j):
        return remote(r_send.at[tn(j)], r_recv.at[t], r_ss.at[j], r_rs.at[t], g, tn(j))

    for j in range(1, TP):
        r_copy(j).start()
    r_recv[t] = r_send[t]
    ph("wait_r")
    for j in range(1, TP):
        src = tn(j)
        remote(r_send.at[src], r_recv.at[src], r_ss.at[j], r_rs.at[src], g, src).wait_recv()
    ph("fin")
    full = jnp.sum(r_recv[...].astype(jnp.float32), axis=0).astype(jnp.bfloat16)
    f_send[...] = full.reshape(8, TOK, HD)

    def f_copy(n, j):
        return remote(
            f_send.at[n], f_recv.at[g, ty], f_ss.at[n, j], f_rs.at[g, ty], zl * 8 + n, tn(j)
        )

    own_half = lax.div(g, 8)

    def each_send(act):
        for n in range(8):
            for j in range(TP):
                if j == 0:
                    @pl.when(zl * 8 + n != g)
                    def _():
                        act(f_copy(n, j))
                else:
                    act(f_copy(n, j))

    each_send(lambda c: c.start())

    @pl.when(zl == own_half)
    def _():
        f_recv[g, ty] = f_send[lax.rem(g, 8)]

    ph("wait_f")
    for gs in range(GEN):
        for ys in range(4):
            def wait_one(gs=gs, ys=ys):
                remote(
                    f_send.at[0], f_recv.at[gs, ys], f_ss.at[0, 0], f_rs.at[gs, ys],
                    gs, ys * 2 + own_half,
                ).wait_recv()

            @pl.when(jnp.logical_not((g == gs) & (t == ys * 2 + own_half)))
            def _():
                wait_one()

    ph("out")
    for c in range(GEN * 4):
        cols = slice(c * HD, (c + 1) * HD)
        block = f_recv[c // 4, c % 4].astype(jnp.float32)
        keep = jnp.where(odd, fin_s[1], fin_s[0]) != 0
        mine = hf_v[:, cols]
        hf_v[:, cols] = jnp.where(keep, mine, mine + block)
    for s in range(4):
        out_ref[s] = hf_v[2 * s:2 * s + 2, :].astype(jnp.bfloat16)

    ph("wait_sends")
    for i in range(1, GEN):
        x_copy(i).wait_send()
        pa_copy(i).wait_send()
        pb_copy(i).wait_send()
        a_copy(i).wait_send()
    unless(own_a, lambda: pa_copy(0).wait_send())
    unless(own_b, lambda: pb_copy(0).wait_send())
    for j in range(1, TP):
        wa_send(j).wait_send()
        wb_send(j).wait_send()
        o_send(j).wait_send()
        r_copy(j).wait_send()
    each_send(lambda c: c.wait_send())
    ph(None)


def shards(
    hidden_in, norm_gain, w_query, key_weight_matrix, value_weight_matrix, bias_query,
    key_bias_vector, value_bias_vector, w_out, key_cache, value_cache, lengths, finished,
):
    any_ = pl.BlockSpec(memory_space=pl.ANY)
    bf16, f32 = jnp.bfloat16, jnp.float32
    dma = pltpu.SemaphoreType.DMA
    return pl.pallas_call(
        kernel,
        out_shape=jax.ShapeDtypeStruct((4, 2, D), bf16),
        in_specs=[any_] * 13,
        out_specs=pl.BlockSpec(memory_space=pltpu.VMEM),
        scratch_shapes=[
            pltpu.VMEM((4, 2, D), bf16),
            pltpu.VMEM((D,), bf16),
            pltpu.VMEM((QW,), bf16),
            pltpu.VMEM((HD,), bf16),
            pltpu.VMEM((HD,), bf16),
            pltpu.SMEM((2,), jnp.int32),
            pltpu.SMEM((2,), jnp.int32),
            pltpu.VMEM((TOK, D), f32),
            pltpu.VMEM((8, 4, TOK, HD), f32),
            pltpu.VMEM((TP, 64, QW), bf16),
            pltpu.VMEM((TP, 64, 2 * HD), bf16),
            pltpu.VMEM((TP, 64, QW), bf16),
            pltpu.VMEM((TP, 64, 2 * HD), bf16),
            pltpu.VMEM((TP, 64, QW), bf16),
            pltpu.VMEM((TP, 64, QW), bf16),
            pltpu.VMEM((2, SLOTS, HD), bf16),
            pltpu.VMEM((2, SLOTS, HD), bf16),
            pltpu.VMEM((NCH, 2 * HD, CHUNK), bf16),
            pltpu.VMEM((8, TOK, 2 * FB), bf16),
            pltpu.VMEM((GEN, TOK, 2 * FB), bf16),
            pltpu.VMEM((GEN, TOK, QW), bf16),
            pltpu.VMEM((GEN, TOK, 2 * HD), bf16),
            pltpu.VMEM((GEN, TOK, QW), bf16),
            pltpu.VMEM((GEN, TOK, 2 * HD), bf16),
            pltpu.VMEM((GEN, TOK, QW), bf16),
            pltpu.VMEM((NCH, 4 * TOK, CHUNK), f32),
            pltpu.VMEM((TP, 64, HD), bf16),
            pltpu.VMEM((TP, 64, HD), bf16),
            pltpu.VMEM((8, TOK, HD), bf16),
            pltpu.VMEM((GEN, 4, TOK, HD), bf16),
            pltpu.VMEM((2, TOK, HD), f32),
            dma((7,)),
            dma((TP, 3)),
            dma((TP,)),
            dma((2, 2, PIECES)),
            dma((GEN,)), dma((GEN,)),
            dma((TP,)), dma((TP,)),
            dma((TP,)), dma((TP,)),
            dma((TP,)), dma((TP,)),
            dma((GEN,)), dma((GEN,)),
            dma((GEN,)), dma((GEN,)),
            dma((GEN,)), dma((GEN,)),
            dma((TP,)), dma((TP,)),
            dma((8, TP)), dma((GEN, 4)),
        ],
        compiler_params=pltpu.CompilerParams(
            collective_id=0, has_side_effects=True, vmem_limit_bytes=60 * 1024 * 1024
        ),
        name="layer",
    )(
        hidden_in, norm_gain, w_query, key_weight_matrix, value_weight_matrix, bias_query,
        key_bias_vector, value_bias_vector, w_out.T, key_cache, value_cache, lengths, finished,
    )


def solution(mesh):
    placed = (
        P(None, "gen", None),
        P(),
        P(("gen", "tp"), None),
        P(("gen", "tp"), None),
        P(("gen", "tp"), None),
        P("tp"),
        P("tp"),
        P("tp"),
        P(None, ("gen", "tp")),
        P("gen", "tp", None, None),
        P("gen", "tp", None, None),
        P("gen"),
        P("gen"),
    )
    return jax.shard_map(
        shards, mesh=mesh, in_specs=placed, out_specs=P(None, "gen", None), check_vma=False
    )
```

```python
import functools
import math

import jax
import jax.numpy as jnp
from jax import lax
from jax.experimental import pallas as pl
from jax.experimental.pallas import tpu as pltpu
from jax.sharding import PartitionSpec as P

NORM_EPS = 1e-06
ROPE_BASE = 1000000.0
MASKED = -1e30
MESH = pl.DeviceIdType.MESH
GEN, TP = 16, 8
TOK = 8
D = 8192
FB = D // GEN
HD = 128
QW = 512
CW = QW + 2 * HD
SLOTS = 16384
CHUNK = 4096
NCH = SLOTS // CHUNK
PIECES = 4
PIECE = SLOTS // PIECES


def peer(g, t):
    return {"gen": g, "tp": t}


def remote(src, dst, send_sem, recv_sem, g, t):
    return pltpu.make_async_remote_copy(
        src_ref=src, dst_ref=dst, send_sem=send_sem, recv_sem=recv_sem,
        device_id=peer(g, t), device_id_type=MESH,
    )


def drained(ref, sem):
    pltpu.make_async_copy(ref, ref, sem).wait()


class Phase:
    def __init__(self):
        self.now = None

    def __call__(self, name):
        if self.now is not None:
            self.now.__exit__(None, None, None)
        self.now = jax.named_scope(name) if name else None
        if name:
            self.now.__enter__()


def kernel(
    hid, gain, wq, wk, wv, bq, bk, bv, wo, kc, vc, lens, fin,
    out_ref,
    h_v, gain_v, bq_v, bk_v, bv_v, lens_s, fin_s, hf_v, m_v,
    wa_stage, wb_stage, wa_full, wb_full, o_stage, o_full, k_v, v_v, kt_v,
    x_send, x_recv, pa_send, pb_send, pa_recv, pb_recv, a_send, a_recv, s_v,
    o_rows, r_send, r_recv, f_send, f_recv, rope_v,
    small_sem, w_sem, kv_sem,
    x_ss, x_rs, wa_ss, wa_rs, wb_ss, wb_rs, o_ss, o_rs, pa_ss, pa_rs, pb_ss, pb_rs,
    a_ss, a_rs, r_ss, r_rs, f_ss, f_rs,
):
    ph = Phase()
    g = lax.axis_index("gen")
    t = lax.axis_index("tp")
    x, zh, core = lax.div(g, 4), lax.rem(lax.div(g, 2), 2), lax.rem(g, 2)
    ty, zl = lax.div(t, 2), lax.rem(t, 2)
    pa = 2 * ty + core
    pb = 2 * x + core

    def gn(i):
        return lax.rem(g + i, GEN)

    def tn(j):
        return lax.rem(t + j, TP)

    def an(j):
        p = lax.rem(pa + j, TP)
        return p, g - core + lax.rem(p, 2), 2 * lax.div(p, 2) + zl

    def bn(j):
        p = lax.rem(pb + j, TP)
        return p, 4 * lax.div(p, 2) + 2 * zh + lax.rem(p, 2), t

    ph("issue")
    barrier = pltpu.get_barrier_semaphore()

    def greet(gg, tt):
        pl.semaphore_signal(barrier, inc=1, device_id=peer(gg, tt), device_id_type=MESH)

    for i in range(1, GEN):
        greet(gn(i), t)
    for j in range(1, TP):
        greet(g, tn(j))
    for k in range(1, 4):
        greet(g - core + (1 - core), lax.rem(t + 2 * k, TP))

    smalls = [
        pltpu.make_async_copy(src, dst, small_sem.at[n])
        for n, (src, dst) in enumerate((
            (hid, h_v), (gain, gain_v), (bq, bq_v), (bk, bk_v), (bv, bv_v), (lens, lens_s), (fin, fin_s),
        ))
    ]
    for c in smalls:
        c.start()

    def wa_copy(j):
        p = lax.rem(pa + j, TP)
        dst = wa_full if j == 0 else wa_stage
        return pltpu.make_async_copy(wq.at[:, pl.ds(p * QW, QW)], dst.at[p], w_sem.at[0])

    def wb_copies(j):
        p = lax.rem(pb + j, TP)
        dst = (wb_full if j == 0 else wb_stage).at[p]
        return [
            pltpu.make_async_copy(src.at[:, pl.ds(p * HD, HD)], dst.at[:, pl.ds(n * HD, HD)], w_sem.at[1])
            for n, src in enumerate((wk, wv))
        ]

    def wo_copy(j):
        p = lax.rem(pa + j, TP)
        dst = o_full if j == 0 else o_stage
        return pltpu.make_async_copy(wo.at[:, pl.ds(p * QW, QW)], dst.at[p], w_sem.at[2])

    for j in range(TP):
        wa_copy(j).start()
        for c in wb_copies(j):
            c.start()

    def kv_copy(n, r, i):
        src, dst = ((kc, k_v), (vc, v_v))[n]
        return pltpu.make_async_copy(
            src.at[r, 0, pl.ds(i * PIECE, PIECE), :],
            dst.at[r, pl.ds(i * PIECE, PIECE), :],
            kv_sem.at[i if n == 0 else PIECES],
        )

    ph("norm")
    smalls[0].wait()
    smalls[1].wait()
    h = jnp.concatenate([h_v[s].astype(jnp.float32) for s in range(4)], axis=0)
    hf_v[...] = h
    scale = lax.rsqrt(jnp.mean(h * h, axis=-1, keepdims=True) + NORM_EPS)
    normed = h * scale * gain_v[...].astype(jnp.float32).reshape(1, D)
    row = lax.broadcasted_iota(jnp.int32, (TOK, HD), 0)
    lane = lax.broadcasted_iota(jnp.int32, (TOK, HD), 1)
    stays = (lane < 64) == (zl == 0)
    for n in range(8):
        for m in range(4):
            c0 = normed[:, (8 * n + m) * HD:(8 * n + m + 1) * HD]
            c1 = normed[:, (8 * n + 4 + m) * HD:(8 * n + 5 + m) * HD]
            moved = pltpu.roll(jnp.where(zl == 0, c1, c0), 64, axis=1)
            both = jnp.where(stays, jnp.where(zl == 0, c0, c1), moved)
            m_v[n, m] = both
            x_send[n, :, m * HD:(m + 1) * HD] = both.astype(jnp.bfloat16)
    for z in range(2):
        for m in range(4):
            block = m_v[2 * m + z, ty].astype(jnp.bfloat16)
            for n in range(4):
                x_send[2 * n + z, :, FB + m * HD:FB + (m + 1) * HD] = block
    x_recv[g] = x_send[lax.div(g, 2)]

    ph("barrier")
    pl.semaphore_wait(barrier, GEN - 1 + TP - 1 + 3)
    ph("send_xw")

    def x_copy(i):
        return remote(x_send.at[lax.div(gn(i), 2)], x_recv.at[g], x_ss, x_rs, gn(i), t)

    def wa_send(j):
        p, gg, tt = an(j)
        return remote(wa_stage.at[p], wa_full.at[pa], wa_ss, wa_rs, gg, tt)

    def wb_send(j):
        p, gg, tt = bn(j)
        return remote(wb_stage.at[p], wb_full.at[pb], wb_ss, wb_rs, gg, tt)

    def o_send(j):
        p, gg, tt = an(j)
        return remote(o_stage.at[p], o_full.at[pa], o_ss, o_rs, gg, tt)

    for i in range(1, GEN):
        x_copy(i).start()
    drained(wa_stage, w_sem.at[0])
    drained(wb_stage, w_sem.at[1])
    for j in range(1, TP):
        wa_send(j).start()
        wb_send(j).start()
    for n in range(2):
        for i in range(PIECES):
            for r in range(2):
                kv_copy(n, r, i).start()
    for j in range(TP):
        wo_copy(j).start()

    ph("rope")
    for c in smalls[2:]:
        c.wait()
    odd = lax.rem(row, 2) == 1
    len8 = jnp.where(odd, lens_s[1], lens_s[0])
    position = (len8 + lax.div(row, 2)).astype(jnp.float32)
    pair = lax.rem(lane, HD // 2).astype(jnp.float32)
    angles = position * jnp.exp(pair * (-2.0 * math.log(ROPE_BASE) / HD))
    rope_v[0] = jnp.cos(angles)
    rope_v[1] = jnp.where(lane < HD // 2, -1.0, 1.0) * jnp.sin(angles)

    ph("turn_k")
    nt = (((1,), (1,)), ((), ()))
    er = lax.broadcasted_iota(jnp.int32, (2 * HD, 2 * HD), 0)
    ec = lax.broadcasted_iota(jnp.int32, (2 * HD, 2 * HD), 1)
    eye = jnp.where(er == ec, 1.0, 0.0).astype(jnp.bfloat16)
    per = PIECE // CHUNK
    for i in range(PIECES):
        drained(k_v.at[:, pl.ds(i * PIECE, PIECE), :], kv_sem.at[i])

        def turn(c, carry):
            at = pl.multiple_of(c * CHUNK, CHUNK)
            keys = jnp.concatenate([k_v[0, pl.ds(at, CHUNK), :], k_v[1, pl.ds(at, CHUNK), :]], axis=1)
            kt_v[c] = lax.dot_general(eye, keys, nt, preferred_element_type=jnp.float32).astype(jnp.bfloat16)
            return carry

        lax.fori_loop(i * per, (i + 1) * per, turn, 0)

    ph("wait_x")
    drained(x_recv.at[pl.ds(0, GEN - 1)], x_rs)
    ph("wait_wa")
    drained(wa_full.at[pl.ds(0, TP - 1)], wa_rs)
    ph("qkv")
    part = jnp.dot(
        x_recv[:, :, :FB].reshape(GEN * TOK, FB), wa_full[...].reshape(FB, QW),
        preferred_element_type=jnp.float32,
    )
    pa_send[...] = part.astype(jnp.bfloat16).reshape(GEN, TOK, QW)

    slot_a = 4 * x + 2 * zh + zl
    slot_b = 4 * ty + 2 * zh + zl

    def pa_copy(i):
        return remote(pa_send.at[gn(i)], pa_recv.at[slot_a], pa_ss, pa_rs, gn(i), pa)

    def pb_copy(i):
        return remote(pb_send.at[gn(i)], pb_recv.at[slot_b], pb_ss, pb_rs, gn(i), pb)

    def unless(own, act):
        @pl.when(jnp.logical_not(own))
        def _():
            act()

    def drained_but(own, ref, sem):
        @pl.when(own)
        def _():
            drained(ref.at[pl.ds(0, GEN - 1)], sem)

        unless(own, lambda: drained(ref, sem))

    own_a = zl == core
    own_b = t == pb
    for i in range(1, GEN):
        pa_copy(i).start()
    unless(own_a, lambda: pa_copy(0).start())

    @pl.when(own_a)
    def _():
        pa_recv[slot_a] = pa_send[g]

    ph("wait_wb")
    drained(wb_full.at[pl.ds(0, TP - 1)], wb_rs)
    ph("kvp")
    part = jnp.dot(
        x_recv[:, :, FB:].reshape(GEN * TOK, FB), wb_full[...].reshape(FB, 2 * HD),
        preferred_element_type=jnp.float32,
    )
    pb_send[...] = part.astype(jnp.bfloat16).reshape(GEN, TOK, 2 * HD)
    for i in range(1, GEN):
        pb_copy(i).start()
    unless(own_b, lambda: pb_copy(0).start())

    @pl.when(own_b)
    def _():
        pb_recv[slot_b] = pb_send[g]

    ph("wait_p")
    drained_but(own_a, pa_recv, pa_rs)
    drained_but(own_b, pb_recv, pb_rs)
    ph("send_o")
    drained(o_stage, w_sem.at[2])
    for j in range(1, TP):
        o_send(j).start()
    ph("wait_kv")
    drained(v_v, kv_sem.at[PIECES])

    ph("head")
    cosine = rope_v[0]
    sine = rope_v[1]

    def rotated(v):
        return v * cosine + pltpu.roll(v, HD // 2, axis=1) * sine

    qs = jnp.sum(pa_recv[...].astype(jnp.float32), axis=0) + bq_v[...].astype(jnp.float32).reshape(1, QW)
    kvs = jnp.sum(pb_recv[...].astype(jnp.float32), axis=0)
    q = jnp.concatenate([rotated(qs[:, n * HD:(n + 1) * HD]) for n in range(4)], axis=0)
    k_new = rotated(kvs[:, :HD] + bk_v[...].astype(jnp.float32).reshape(1, HD)).astype(jnp.bfloat16)
    v_new = (kvs[:, HD:] + bv_v[...].astype(jnp.float32).reshape(1, HD)).astype(jnp.bfloat16)
    qrow = lax.broadcasted_iota(jnp.int32, (4 * TOK, HD), 0)
    q_odd = lax.rem(qrow, 2) == 1
    q_both = jnp.concatenate(
        [jnp.where(q_odd, 0.0, q), jnp.where(q_odd, q, 0.0)], axis=1
    ).astype(jnp.bfloat16)
    q16 = q.astype(jnp.bfloat16)
    qlen = jnp.where(q_odd, lens_s[1], lens_s[0])
    place = lax.broadcasted_iota(jnp.int32, (4 * TOK, HD), 1)

    fresh = lax.dot_general(q16, k_new, nt, preferred_element_type=jnp.float32)
    fq = lax.rem(lax.broadcasted_iota(jnp.int32, (4 * TOK, TOK), 0), TOK)
    fk = lax.broadcasted_iota(jnp.int32, (4 * TOK, TOK), 1)
    seen = (lax.rem(fq, 2) == lax.rem(fk, 2)) & (lax.div(fk, 2) <= lax.div(fq, 2))
    fresh = jnp.where(seen, fresh, MASKED)

    def score(c, top):
        s = jnp.dot(q_both, kt_v[c], preferred_element_type=jnp.float32)
        rest = qlen - c * CHUNK
        for n in range(CHUNK // HD):
            part = jnp.where(place < rest - n * HD, s[:, n * HD:(n + 1) * HD], MASKED)
            s_v[c, :, n * HD:(n + 1) * HD] = part
            top = jnp.maximum(top, part)
        return top

    ph("score")
    top = lax.fori_loop(0, NCH, score, jnp.full((4 * TOK, HD), MASKED, jnp.float32))
    top = jnp.maximum(jnp.max(top, axis=1, keepdims=True), jnp.max(fresh, axis=1, keepdims=True))
    to_exp = math.log2(math.e) / math.sqrt(HD)

    def weigh(c, carry):
        total, acc = carry
        at = pl.multiple_of(c * CHUNK, CHUNK)
        w = jnp.exp2((s_v[c] - top) * to_exp)
        for n in range(CHUNK // HD):
            total = total + w[:, n * HD:(n + 1) * HD]
        values = jnp.concatenate([v_v[0, pl.ds(at, CHUNK), :], v_v[1, pl.ds(at, CHUNK), :]], axis=1)
        acc = acc + jnp.dot(w.astype(jnp.bfloat16), values, preferred_element_type=jnp.float32)
        return total, acc

    ph("weigh")
    total, acc = lax.fori_loop(
        0, NCH, weigh,
        (jnp.zeros((4 * TOK, HD), jnp.float32), jnp.zeros((4 * TOK, 2 * HD), jnp.float32)),
    )
    ph("att_end")
    fw = jnp.exp2((fresh - top) * to_exp)
    denom = jnp.sum(total, axis=1, keepdims=True) + jnp.sum(fw, axis=1, keepdims=True)
    num = jnp.where(q_odd, acc[:, HD:], acc[:, :HD])
    num = num + jnp.dot(fw.astype(jnp.bfloat16), v_new, preferred_element_type=jnp.float32)
    att = num / denom
    a_send[...] = jnp.concatenate([att[n * TOK:(n + 1) * TOK] for n in range(4)], axis=1).astype(jnp.bfloat16)

    def a_copy(i):
        k = lax.rem(slot_a + i, GEN)
        gg = 4 * lax.div(k, 4) + 2 * lax.rem(lax.div(k, 2), 2) + zl
        return remote(a_send, a_recv.at[g], a_ss, a_rs, gg, 2 * ty + lax.rem(k, 2))

    for i in range(1, GEN):
        a_copy(i).start()
    unless(own_a, lambda: a_copy(0).start())

    @pl.when(own_a)
    def _():
        a_recv[g] = a_send[...]

    ph("wait_o")
    drained(o_full.at[pl.ds(0, TP - 1)], o_rs)
    ph("wait_a")
    drained_but(own_a, a_recv, a_rs)

    ph("outmm")
    a_all = a_recv[...].reshape(GEN * TOK, QW)
    o_all = o_full[...].reshape(QW, QW)
    outp = lax.dot_general(a_all, o_all, nt, preferred_element_type=jnp.float32)
    def group(yy, cc, n):
        return 4 * lax.rem(x + yy + 2 * n, 4) + 2 * lax.rem(zh + lax.div(yy, 2), 2) + cc

    o_rows[...] = outp.reshape(GEN, TOK, QW)
    for p in range(TP):
        for n in range(2):
            r_send[p, n] = o_rows[group(p // 2, p % 2, n)].astype(jnp.bfloat16)

    def r_copy(j):
        p, gg, tt = an(j)
        return remote(r_send.at[p], r_recv.at[pa], r_ss, r_rs, gg, tt)

    for j in range(1, TP):
        r_copy(j).start()
    r_recv[pa] = r_send[pa]
    ph("wait_r")
    drained(r_recv.at[pl.ds(0, TP - 1)], r_rs)
    ph("fin")
    full = jnp.sum(r_recv[...].astype(jnp.float32), axis=0).astype(jnp.bfloat16)
    f_send[...] = full
    slot_f = 4 * x + 2 * zh + zl
    own_f = ty == 0

    def f_copy(n, j):
        return remote(f_send.at[n], f_recv.at[slot_f], f_ss, f_rs, group(ty, core, n), tn(j))

    for j in range(1, TP):
        for n in range(2):
            f_copy(n, j).start()
    f_copy(1, 0).start()
    unless(own_f, lambda: f_copy(0, 0).start())

    @pl.when(own_f)
    def _():
        f_recv[slot_f] = f_send[0]

    ph("wait_f")
    drained_but(own_f, f_recv, f_rs)

    ph("out")
    keep = jnp.where(odd, fin_s[1], fin_s[0]) != 0
    first = lane < 64
    for n in range(8):
        for m in range(4):
            z0 = f_recv[2 * n, :, m * HD:(m + 1) * HD].astype(jnp.float32)
            z1 = f_recv[2 * n + 1, :, m * HD:(m + 1) * HD].astype(jnp.float32)
            c0 = jnp.where(first, z0, pltpu.roll(z1, 64, axis=1))
            c1 = jnp.where(first, pltpu.roll(z0, 64, axis=1), z1)
            for block, c in ((c0, 8 * n + m), (c1, 8 * n + 4 + m)):
                mine = hf_v[:, c * HD:(c + 1) * HD]
                hf_v[:, c * HD:(c + 1) * HD] = jnp.where(keep, mine, mine + block)
    for s in range(4):
        out_ref[s] = hf_v[2 * s:2 * s + 2, :].astype(jnp.bfloat16)

    ph("wait_sends")
    drained(x_recv.at[pl.ds(0, GEN - 1)], x_ss)
    drained(wa_full.at[pl.ds(0, TP - 1)], wa_ss)
    drained(wb_full.at[pl.ds(0, TP - 1)], wb_ss)
    drained(o_full.at[pl.ds(0, TP - 1)], o_ss)
    drained_but(own_a, pa_recv, pa_ss)
    drained_but(own_b, pb_recv, pb_ss)
    drained_but(own_a, a_recv, a_ss)
    drained(r_recv.at[pl.ds(0, TP - 1)], r_ss)
    drained_but(own_f, f_recv, f_ss)
    ph(None)


def shards(
    hidden_in, norm_gain, w_query, key_weight_matrix, value_weight_matrix, bias_query,
    key_bias_vector, value_bias_vector, w_out, key_cache, value_cache, lengths, finished,
):
    any_ = pl.BlockSpec(memory_space=pl.ANY)
    bf16, f32 = jnp.bfloat16, jnp.float32
    dma = pltpu.SemaphoreType.DMA
    return pl.pallas_call(
        kernel,
        out_shape=jax.ShapeDtypeStruct((4, 2, D), bf16),
        in_specs=[any_] * 13,
        out_specs=pl.BlockSpec(memory_space=pltpu.VMEM),
        scratch_shapes=[
            pltpu.VMEM((4, 2, D), bf16),
            pltpu.VMEM((D,), bf16),
            pltpu.VMEM((QW,), bf16),
            pltpu.VMEM((HD,), bf16),
            pltpu.VMEM((HD,), bf16),
            pltpu.SMEM((2,), jnp.int32),
            pltpu.SMEM((2,), jnp.int32),
            pltpu.VMEM((TOK, D), f32),
            pltpu.VMEM((8, 4, TOK, HD), f32),
            pltpu.VMEM((TP, 64, QW), bf16),
            pltpu.VMEM((TP, 64, 2 * HD), bf16),
            pltpu.VMEM((TP, 64, QW), bf16),
            pltpu.VMEM((TP, 64, 2 * HD), bf16),
            pltpu.VMEM((TP, 64, QW), bf16),
            pltpu.VMEM((TP, 64, QW), bf16),
            pltpu.VMEM((2, SLOTS, HD), bf16),
            pltpu.VMEM((2, SLOTS, HD), bf16),
            pltpu.VMEM((NCH, 2 * HD, CHUNK), bf16),
            pltpu.VMEM((8, TOK, 2 * FB), bf16),
            pltpu.VMEM((GEN, TOK, 2 * FB), bf16),
            pltpu.VMEM((GEN, TOK, QW), bf16),
            pltpu.VMEM((GEN, TOK, 2 * HD), bf16),
            pltpu.VMEM((GEN, TOK, QW), bf16),
            pltpu.VMEM((GEN, TOK, 2 * HD), bf16),
            pltpu.VMEM((TOK, QW), bf16),
            pltpu.VMEM((GEN, TOK, QW), bf16),
            pltpu.VMEM((NCH, 4 * TOK, CHUNK), f32),
            pltpu.VMEM((GEN, TOK, QW), f32),
            pltpu.VMEM((TP, 2, TOK, QW), bf16),
            pltpu.VMEM((TP, 2, TOK, QW), bf16),
            pltpu.VMEM((2, TOK, QW), bf16),
            pltpu.VMEM((GEN, TOK, QW), bf16),
            pltpu.VMEM((2, TOK, HD), f32),
            dma((7,)),
            dma((3,)),
            dma((PIECES + 1,)),
        ] + [dma(())] * 18,
        compiler_params=pltpu.CompilerParams(
            collective_id=0, has_side_effects=True, vmem_limit_bytes=60 * 1024 * 1024
        ),
        name="layer",
    )(
        hidden_in, norm_gain, w_query, key_weight_matrix, value_weight_matrix, bias_query,
        key_bias_vector, value_bias_vector, w_out.T, key_cache, value_cache, lengths, finished,
    )


def solution(mesh):
    placed = (
        P(None, "gen", None),
        P(),
        P(("gen", "tp"), None),
        P(("gen", "tp"), None),
        P(("gen", "tp"), None),
        P("tp"),
        P("tp"),
        P("tp"),
        P(None, ("gen", "tp")),
        P("gen", "tp", None, None),
        P("gen", "tp", None, None),
        P("gen"),
        P("gen"),
    )
    return jax.shard_map(
        shards, mesh=mesh, in_specs=placed, out_specs=P(None, "gen", None), check_vma=False
    )
```

```python
import functools
import math

import jax
import jax.numpy as jnp
from jax import lax
from jax.experimental import pallas as pl
from jax.experimental.pallas import tpu as pltpu
from jax.sharding import PartitionSpec as P

NORM_EPS = 1e-06
ROPE_BASE = 1000000.0
MASKED = -1e30
MESH = pl.DeviceIdType.MESH
GEN, TP = 16, 8
TOK = 8
D = 8192
FB = D // GEN
HD = 128
QW = 512
CW = QW + 2 * HD
SLOTS = 16384
CHUNK = 8192
NCH = SLOTS // CHUNK
PIECES = 2
PIECE = SLOTS // PIECES
FAR = sorted(
    ((dx, dz, d) for dx in range(4) for dz in range(2) for d in (1, 0)),
    key=lambda o: -(min(o[0], 4 - o[0]) + 2 * o[1]),
)
NEAR = [(d, dc) for d in (2, 1, 3, 0) for dc in (1, 0)]


def peer(g, t):
    return {"gen": g, "tp": t}


def remote(src, dst, send_sem, recv_sem, g, t):
    return pltpu.make_async_remote_copy(
        src_ref=src, dst_ref=dst, send_sem=send_sem, recv_sem=recv_sem,
        device_id=peer(g, t), device_id_type=MESH,
    )


def drained(ref, sem):
    pltpu.make_async_copy(ref, ref, sem).wait()


class Phase:
    def __init__(self):
        self.now = None

    def __call__(self, name):
        if self.now is not None:
            self.now.__exit__(None, None, None)
        self.now = jax.named_scope(name) if name else None
        if name:
            self.now.__enter__()


def kernel(
    hid, gain, wq, wk, wv, bq, bk, bv, wo, kc, vc, lens, fin,
    out_ref,
    h_v, gain_v, bq_v, bk_v, bv_v, lens_s, fin_s, hf_v, m_v,
    wa_stage, wb_stage, wa_full, wb_full, o_stage, o_full, k_v, v_v, kt_v,
    xa_send, xa_recv, xb_send, xb_recv, pa_send, pb_send, pa_recv, pb_recv, a_send, a_recv, s_v, w_v,
    o_rows, r_send, r_recv, f_send, f_recv, rope_v,
    small_sem, w_sem, kv_sem,
    xa_ss, xa_rs, xb_ss, xb_rs, wa_ss, wa_rs, wb_ss, wb_rs, o_ss, o_rs, pa_ss, pa_rs, pb_ss, pb_rs,
    a_ss, a_rs, r_ss, r_rs, f_ss, f_rs,
):
    ph = Phase()
    g = lax.axis_index("gen")
    t = lax.axis_index("tp")
    x, zh, core = lax.div(g, 4), lax.rem(lax.div(g, 2), 2), lax.rem(g, 2)
    ty, zl = lax.div(t, 2), lax.rem(t, 2)
    pa = 2 * ty + core
    pb = 2 * lax.rem(x + ty, 4) + core

    def gn(dx, dz, dc):
        return 4 * lax.rem(x + dx, 4) + 2 * lax.rem(zh + dz, 2) + lax.rem(core + dc, 2)

    def an(o):
        yy, cc = lax.rem(ty + o[0], 4), lax.rem(core + o[1], 2)
        return 2 * yy + cc, g - core + cc, 2 * yy + zl

    def bn(o):
        xx, cc = lax.rem(x + o[0], 4), lax.rem(core + o[1], 2)
        return 2 * lax.rem(xx + ty, 4) + cc, 4 * xx + 2 * zh + cc, t

    ph("issue")
    smalls = [
        pltpu.make_async_copy(src, dst, small_sem.at[n])
        for n, (src, dst) in enumerate((
            (hid, h_v), (gain, gain_v), (bq, bq_v), (bk, bk_v), (bv, bv_v), (lens, lens_s), (fin, fin_s),
        ))
    ]
    for c in smalls[:2]:
        c.start()
    barrier = pltpu.get_barrier_semaphore()

    def greet(gg, tt):
        pl.semaphore_signal(barrier, inc=1, device_id=peer(gg, tt), device_id_type=MESH)

    for o in FAR[:-1]:
        greet(gn(*o), t)
    for j in range(1, TP):
        greet(g, lax.rem(t + j, TP))
    for k in range(1, 4):
        greet(g - core + (1 - core), lax.rem(t + 2 * k, TP))

    def wa_copy(o):
        p = an(o)[0]
        dst = wa_full if o == (0, 0) else wa_stage
        return pltpu.make_async_copy(wq.at[:, pl.ds(p * QW, QW)], dst.at[p], w_sem.at[0])

    def wb_copies(o):
        p = bn(o)[0]
        slot = 2 * x + core if o == (0, 0) else p
        dst = (wb_full if o == (0, 0) else wb_stage).at[slot]
        return [
            pltpu.make_async_copy(src.at[:, pl.ds(p * HD, HD)], dst.at[:, pl.ds(n * HD, HD)], w_sem.at[1])
            for n, src in enumerate((wk, wv))
        ]

    def wo_copy(o):
        p = an(o)[0]
        dst = o_full if o == (0, 0) else o_stage
        return pltpu.make_async_copy(wo.at[:, pl.ds(p * QW, QW)], dst.at[p], w_sem.at[2])

    for o in NEAR:
        wa_copy(o).start()
        for c in wb_copies(o):
            c.start()
    for c in smalls[2:]:
        c.start()

    def kv_copy(n, r, i):
        src, dst = ((kc, k_v), (vc, v_v))[n]
        return pltpu.make_async_copy(
            src.at[r, 0, pl.ds(i * PIECE, PIECE), :],
            dst.at[r, pl.ds(i * PIECE, PIECE), :],
            kv_sem.at[i if n == 0 else PIECES],
        )

    ph("norm")
    smalls[0].wait()
    smalls[1].wait()
    h = jnp.concatenate([h_v[s].astype(jnp.float32) for s in range(4)], axis=0)
    hf_v[...] = h
    scale = lax.rsqrt(jnp.mean(h * h, axis=-1, keepdims=True) + NORM_EPS)
    normed = h * scale * gain_v[...].astype(jnp.float32).reshape(1, D)
    row = lax.broadcasted_iota(jnp.int32, (TOK, HD), 0)
    lane = lax.broadcasted_iota(jnp.int32, (TOK, HD), 1)
    stays = (lane < 64) == (zl == 0)
    for n in range(8):
        for m in range(4):
            c0 = normed[:, (8 * n + m) * HD:(8 * n + m + 1) * HD]
            c1 = normed[:, (8 * n + 4 + m) * HD:(8 * n + 5 + m) * HD]
            moved = pltpu.roll(jnp.where(zl == 0, c1, c0), 64, axis=1)
            both = jnp.where(stays, jnp.where(zl == 0, c0, c1), moved)
            m_v[n, m] = both
            xa_send[n, :, m * HD:(m + 1) * HD] = both.astype(jnp.bfloat16)
    for z in range(2):
        for m in range(4):
            xb_send[z, :, m * HD:(m + 1) * HD] = m_v[2 * m + z, ty].astype(jnp.bfloat16)
    xa_recv[g] = xa_send[2 * x + zh]
    xb_recv[g] = xb_send[zh]

    ph("barrier")
    pl.semaphore_wait(barrier, GEN - 1 + TP - 1 + 3)
    ph("send_xw")

    def xa_copy(o):
        gg = gn(*o)
        return remote(xa_send.at[lax.div(gg, 2)], xa_recv.at[g], xa_ss, xa_rs, gg, t)

    def xb_copy(o):
        gg = gn(*o)
        return remote(xb_send.at[lax.rem(lax.div(gg, 2), 2)], xb_recv.at[g], xb_ss, xb_rs, gg, t)

    def wa_send(o):
        p, gg, tt = an(o)
        return remote(wa_stage.at[p], wa_full.at[pa], wa_ss, wa_rs, gg, tt)

    def wb_send(o):
        p, gg, tt = bn(o)
        return remote(wb_stage.at[p], wb_full.at[2 * x + core], wb_ss, wb_rs, gg, tt)

    def o_send(o):
        p, gg, tt = an(o)
        return remote(o_stage.at[p], o_full.at[pa], o_ss, o_rs, gg, tt)

    drained(wa_stage, w_sem.at[0])
    for o in NEAR[:-1]:
        wa_send(o).start()
    for o in FAR[:-1]:
        xa_copy(o).start()
    for o in FAR[:-1]:
        xb_copy(o).start()
    drained(wb_stage, w_sem.at[1])
    for o in NEAR[:-1]:
        wb_send(o).start()
    for n in range(2):
        for i in range(PIECES):
            for r in range(2):
                kv_copy(n, r, i).start()
    for o in NEAR:
        wo_copy(o).start()

    ph("rope")
    for c in smalls[2:]:
        c.wait()
    odd = lax.rem(row, 2) == 1
    len8 = jnp.where(odd, lens_s[1], lens_s[0])
    position = (len8 + lax.div(row, 2)).astype(jnp.float32)
    pair = lax.rem(lane, HD // 2).astype(jnp.float32)
    angles = position * jnp.exp(pair * (-2.0 * math.log(ROPE_BASE) / HD))
    rope_v[0] = jnp.cos(angles)
    rope_v[1] = jnp.where(lane < HD // 2, -1.0, 1.0) * jnp.sin(angles)

    ph("turn_k")
    nt = (((1,), (1,)), ((), ()))
    er = lax.broadcasted_iota(jnp.int32, (2 * HD, 2 * HD), 0)
    ec = lax.broadcasted_iota(jnp.int32, (2 * HD, 2 * HD), 1)
    eye = jnp.where(er == ec, 1.0, 0.0).astype(jnp.bfloat16)
    per = PIECE // CHUNK
    for i in range(PIECES):
        drained(k_v.at[:, pl.ds(i * PIECE, PIECE), :], kv_sem.at[i])

        def turn(c, carry):
            at = pl.multiple_of(c * CHUNK, CHUNK)
            keys = jnp.concatenate([k_v[0, pl.ds(at, CHUNK), :], k_v[1, pl.ds(at, CHUNK), :]], axis=1)
            kt_v[c] = lax.dot_general(eye, keys, nt, preferred_element_type=jnp.float32).astype(jnp.bfloat16)
            return carry

        lax.fori_loop(i * per, (i + 1) * per, turn, 0)

    ph("wait_x")
    drained(xa_recv.at[pl.ds(0, GEN - 1)], xa_rs)
    slot_a = 4 * x + 2 * zh + zl
    slot_b = 4 * ty + 2 * zh + zl
    own_a = zl == core
    own_b = own_a & (x == 0)

    def pa_copy(o):
        gg = gn(*o)
        return remote(pa_send.at[gg], pa_recv.at[slot_a], pa_ss, pa_rs, gg, pa)

    def pb_copy(o):
        gg = gn(*o)
        return remote(pb_send.at[gg], pb_recv.at[slot_b], pb_ss, pb_rs, gg, pb)

    def unless(own, act):
        @pl.when(jnp.logical_not(own))
        def _():
            act()

    def drained_but(own, ref, sem):
        @pl.when(own)
        def _():
            drained(ref.at[pl.ds(0, GEN - 1)], sem)

        unless(own, lambda: drained(ref, sem))

    ph("wait_wa")
    drained(wa_full.at[pl.ds(0, TP - 1)], wa_rs)
    ph("qkv")
    part = jnp.dot(
        xa_recv[...].reshape(GEN * TOK, FB), wa_full[...].reshape(FB, QW),
        preferred_element_type=jnp.float32,
    )
    pa_send[...] = part.astype(jnp.bfloat16).reshape(GEN, TOK, QW)
    for o in FAR[:-1]:
        pa_copy(o).start()
    unless(own_a, lambda: pa_copy(FAR[-1]).start())

    @pl.when(own_a)
    def _():
        pa_recv[slot_a] = pa_send[g]

    ph("wait_wb")
    drained(xb_recv.at[pl.ds(0, GEN - 1)], xb_rs)
    drained(wb_full.at[pl.ds(0, TP - 1)], wb_rs)
    ph("kvp")
    part = jnp.dot(
        xb_recv[...].reshape(GEN * TOK, FB), wb_full[...].reshape(FB, 2 * HD),
        preferred_element_type=jnp.float32,
    )
    pb_send[...] = part.astype(jnp.bfloat16).reshape(GEN, TOK, 2 * HD)
    for o in FAR[:-1]:
        pb_copy(o).start()
    unless(own_b, lambda: pb_copy(FAR[-1]).start())

    @pl.when(own_b)
    def _():
        pb_recv[slot_b] = pb_send[g]

    ph("wait_p")
    drained_but(own_a, pa_recv, pa_rs)
    ph("send_o")
    drained(o_stage, w_sem.at[2])
    for o in NEAR[:-1]:
        o_send(o).start()

    ph("head")
    cosine = rope_v[0]
    sine = rope_v[1]

    def rotated(v):
        return v * cosine + pltpu.roll(v, HD // 2, axis=1) * sine

    qs = jnp.sum(pa_recv[...].astype(jnp.float32), axis=0) + bq_v[...].astype(jnp.float32).reshape(1, QW)
    q = jnp.concatenate([rotated(qs[:, n * HD:(n + 1) * HD]) for n in range(4)], axis=0)
    qrow = lax.broadcasted_iota(jnp.int32, (4 * TOK, HD), 0)
    q_odd = lax.rem(qrow, 2) == 1
    q_both = jnp.concatenate(
        [jnp.where(q_odd, 0.0, q), jnp.where(q_odd, q, 0.0)], axis=1
    ).astype(jnp.bfloat16)
    q16 = q.astype(jnp.bfloat16)
    qlen = jnp.where(q_odd, lens_s[1], lens_s[0])
    place = lax.broadcasted_iota(jnp.int32, (4 * TOK, HD), 1)

    def score(c, top):
        s = jnp.dot(q_both, kt_v[c], preferred_element_type=jnp.float32)
        rest = qlen - c * CHUNK
        for n in range(CHUNK // HD):
            part = jnp.where(place < rest - n * HD, s[:, n * HD:(n + 1) * HD], MASKED)
            s_v[c, :, n * HD:(n + 1) * HD] = part
            top = jnp.maximum(top, part)
        return top

    ph("score")
    top = lax.fori_loop(0, NCH, score, jnp.full((4 * TOK, HD), MASKED, jnp.float32))
    ph("wait_pb")
    drained_but(own_b, pb_recv, pb_rs)
    drained(v_v, kv_sem.at[PIECES])
    ph("fresh")
    kvs = jnp.sum(pb_recv[...].astype(jnp.float32), axis=0)
    k_new = rotated(kvs[:, :HD] + bk_v[...].astype(jnp.float32).reshape(1, HD)).astype(jnp.bfloat16)
    v_new = (kvs[:, HD:] + bv_v[...].astype(jnp.float32).reshape(1, HD)).astype(jnp.bfloat16)
    fresh = lax.dot_general(q16, k_new, nt, preferred_element_type=jnp.float32)
    fq = lax.rem(lax.broadcasted_iota(jnp.int32, (4 * TOK, TOK), 0), TOK)
    fk = lax.broadcasted_iota(jnp.int32, (4 * TOK, TOK), 1)
    seen = (lax.rem(fq, 2) == lax.rem(fk, 2)) & (lax.div(fk, 2) <= lax.div(fq, 2))
    fresh = jnp.where(seen, fresh, MASKED)

    top = jnp.maximum(jnp.max(top, axis=1, keepdims=True), jnp.max(fresh, axis=1, keepdims=True))
    to_exp = math.log2(math.e) / math.sqrt(HD)

    def weights(c, total):
        w = jnp.exp2((s_v[c] - top) * to_exp)
        for n in range(CHUNK // HD):
            total = total + w[:, n * HD:(n + 1) * HD]
        return w.astype(jnp.bfloat16), total

    def weighed(c, w, acc):
        at = pl.multiple_of(c * CHUNK, CHUNK)
        values = jnp.concatenate([v_v[0, pl.ds(at, CHUNK), :], v_v[1, pl.ds(at, CHUNK), :]], axis=1)
        return acc + jnp.dot(w, values, preferred_element_type=jnp.float32)

    ph("weigh")
    def step(c, carry):
        total, acc = carry
        w, total = weights(c, total)
        return total, weighed(c, w, acc)

    total, acc = lax.fori_loop(
        0, NCH, step,
        (jnp.zeros((4 * TOK, HD), jnp.float32), jnp.zeros((4 * TOK, 2 * HD), jnp.float32)),
    )
    ph("att_end")
    fw = jnp.exp2((fresh - top) * to_exp)
    denom = jnp.sum(total, axis=1, keepdims=True) + jnp.sum(fw, axis=1, keepdims=True)
    num = jnp.where(q_odd, acc[:, HD:], acc[:, :HD])
    num = num + jnp.dot(fw.astype(jnp.bfloat16), v_new, preferred_element_type=jnp.float32)
    att = num / denom
    a_send[...] = jnp.concatenate([att[n * TOK:(n + 1) * TOK] for n in range(4)], axis=1).astype(jnp.bfloat16)

    def a_copy(o):
        dx, dz, d = o
        gg = 4 * lax.rem(x + dx, 4) + 2 * lax.rem(zh + dz, 2) + zl
        return remote(a_send, a_recv.at[g], a_ss, a_rs, gg, 2 * ty + lax.rem(zl + d, 2))

    for o in FAR[:-1]:
        a_copy(o).start()
    unless(own_a, lambda: a_copy(FAR[-1]).start())

    @pl.when(own_a)
    def _():
        a_recv[g] = a_send[...]

    ph("wait_o")
    drained(o_full.at[pl.ds(0, TP - 1)], o_rs)
    ph("wait_a")
    drained_but(own_a, a_recv, a_rs)

    ph("outmm")
    a_all = a_recv[...].reshape(GEN * TOK, QW)
    o_all = o_full[...].reshape(QW, QW)
    outp = lax.dot_general(a_all, o_all, nt, preferred_element_type=jnp.float32)
    def group(yy, cc, n):
        return 4 * lax.rem(x + yy + 2 * n, 4) + 2 * lax.rem(zh + lax.div(yy, 2), 2) + cc

    o_rows[...] = outp.reshape(GEN, TOK, QW)
    for p in range(TP):
        for n in range(2):
            r_send[n, p] = o_rows[group(p // 2, p % 2, n)].astype(jnp.bfloat16)

    def r_copy(o, n):
        p, gg, tt = an(o)
        return remote(r_send.at[n, p], r_recv.at[n, pa], r_ss, r_rs.at[n], gg, tt)

    for n in (1, 0):
        for o in NEAR[:-1]:
            r_copy(o, n).start()
        r_recv[n, pa] = r_send[n, pa]
    slot_f = 4 * x + 2 * zh + zl
    own_f = ty == 0

    def f_copy(o, n):
        tt = 2 * lax.rem(ty + o[0], 4) + lax.rem(zl + o[1], 2)
        return remote(f_send.at[n], f_recv.at[slot_f], f_ss, f_rs, group(ty, core, n), tt)

    for n in (1, 0):
        ph(f"wait_r{n}")
        drained(r_recv.at[n, pl.ds(0, TP - 1)], r_rs.at[n])
        ph(f"fin{n}")
        f_send[n] = jnp.sum(r_recv[n].astype(jnp.float32), axis=0).astype(jnp.bfloat16)
        for o in NEAR[:-1]:
            f_copy(o, n).start()
        if n == 1:
            f_copy(NEAR[-1], 1).start()
        else:
            unless(own_f, lambda: f_copy(NEAR[-1], 0).start())

    @pl.when(own_f)
    def _():
        f_recv[slot_f] = f_send[0]

    ph("wait_f")
    drained_but(own_f, f_recv, f_rs)

    ph("out")
    keep = jnp.where(odd, fin_s[1], fin_s[0]) != 0
    first = lane < 64
    for n in range(8):
        for m in range(4):
            z0 = f_recv[2 * n, :, m * HD:(m + 1) * HD].astype(jnp.float32)
            z1 = f_recv[2 * n + 1, :, m * HD:(m + 1) * HD].astype(jnp.float32)
            c0 = jnp.where(first, z0, pltpu.roll(z1, 64, axis=1))
            c1 = jnp.where(first, pltpu.roll(z0, 64, axis=1), z1)
            for block, c in ((c0, 8 * n + m), (c1, 8 * n + 4 + m)):
                mine = hf_v[:, c * HD:(c + 1) * HD]
                hf_v[:, c * HD:(c + 1) * HD] = jnp.where(keep, mine, mine + block)
    for s in range(4):
        out_ref[s] = hf_v[2 * s:2 * s + 2, :].astype(jnp.bfloat16)

    ph("wait_sends")
    drained(xa_recv.at[pl.ds(0, GEN - 1)], xa_ss)
    drained(xb_recv.at[pl.ds(0, GEN - 1)], xb_ss)
    drained(wa_full.at[pl.ds(0, TP - 1)], wa_ss)
    drained(wb_full.at[pl.ds(0, TP - 1)], wb_ss)
    drained(o_full.at[pl.ds(0, TP - 1)], o_ss)
    drained_but(own_a, pa_recv, pa_ss)
    drained_but(own_b, pb_recv, pb_ss)
    drained_but(own_a, a_recv, a_ss)
    drained(r_recv.at[:, pl.ds(0, TP - 1)], r_ss)
    drained_but(own_f, f_recv, f_ss)
    ph(None)


def shards(
    hidden_in, norm_gain, w_query, key_weight_matrix, value_weight_matrix, bias_query,
    key_bias_vector, value_bias_vector, w_out, key_cache, value_cache, lengths, finished,
):
    any_ = pl.BlockSpec(memory_space=pl.ANY)
    bf16, f32 = jnp.bfloat16, jnp.float32
    dma = pltpu.SemaphoreType.DMA
    return pl.pallas_call(
        kernel,
        out_shape=pltpu.VMEM((4, 2, D), bf16),
        in_specs=[any_] * 13,
        out_specs=pl.BlockSpec(memory_space=pltpu.VMEM),
        scratch_shapes=[
            pltpu.VMEM((4, 2, D), bf16),
            pltpu.VMEM((D,), bf16),
            pltpu.VMEM((QW,), bf16),
            pltpu.VMEM((HD,), bf16),
            pltpu.VMEM((HD,), bf16),
            pltpu.SMEM((2,), jnp.int32),
            pltpu.SMEM((2,), jnp.int32),
            pltpu.VMEM((TOK, D), f32),
            pltpu.VMEM((8, 4, TOK, HD), f32),
            pltpu.VMEM((TP, 64, QW), bf16),
            pltpu.VMEM((TP, 64, 2 * HD), bf16),
            pltpu.VMEM((TP, 64, QW), bf16),
            pltpu.VMEM((TP, 64, 2 * HD), bf16),
            pltpu.VMEM((TP, 64, QW), bf16),
            pltpu.VMEM((TP, 64, QW), bf16),
            pltpu.VMEM((2, SLOTS, HD), bf16),
            pltpu.VMEM((2, SLOTS, HD), bf16),
            pltpu.VMEM((NCH, 2 * HD, CHUNK), bf16),
            pltpu.VMEM((8, TOK, FB), bf16),
            pltpu.VMEM((GEN, TOK, FB), bf16),
            pltpu.VMEM((2, TOK, FB), bf16),
            pltpu.VMEM((GEN, TOK, FB), bf16),
            pltpu.VMEM((GEN, TOK, QW), bf16),
            pltpu.VMEM((GEN, TOK, 2 * HD), bf16),
            pltpu.VMEM((GEN, TOK, QW), bf16),
            pltpu.VMEM((GEN, TOK, 2 * HD), bf16),
            pltpu.VMEM((TOK, QW), bf16),
            pltpu.VMEM((GEN, TOK, QW), bf16),
            pltpu.VMEM((NCH, 4 * TOK, CHUNK), f32),
            pltpu.VMEM((2, 4 * TOK, CHUNK), bf16),
            pltpu.VMEM((GEN, TOK, QW), f32),
            pltpu.VMEM((2, TP, TOK, QW), bf16),
            pltpu.VMEM((2, TP, TOK, QW), bf16),
            pltpu.VMEM((2, TOK, QW), bf16),
            pltpu.VMEM((GEN, TOK, QW), bf16),
            pltpu.VMEM((2, TOK, HD), f32),
            dma((7,)),
            dma((3,)),
            dma((PIECES + 1,)),
        ] + [dma(())] * 17 + [dma((2,))] + [dma(())] * 2,
        compiler_params=pltpu.CompilerParams(
            collective_id=0, has_side_effects=True, vmem_limit_bytes=60 * 1024 * 1024
        ),
        name="layer",
    )(
        hidden_in, norm_gain, w_query, key_weight_matrix, value_weight_matrix, bias_query,
        key_bias_vector, value_bias_vector, w_out.T, key_cache, value_cache, lengths, finished,
    )


def solution(mesh):
    placed = (
        P(None, "gen", None),
        P(),
        P(("gen", "tp"), None),
        P(("gen", "tp"), None),
        P(("gen", "tp"), None),
        P("tp"),
        P("tp"),
        P("tp"),
        P(None, ("gen", "tp")),
        P("gen", "tp", None, None),
        P("gen", "tp", None, None),
        P("gen"),
        P("gen"),
    )
    return jax.shard_map(
        shards, mesh=mesh, in_specs=placed, out_specs=P(None, "gen", None), check_vma=False
    )
```
